8 devices in a mesh: dp: 8 (over z, y, x, core).
Axes of the slice: x: 2, y: 2, z: 1, core: 2. Of those that a mesh axis runs over, the one named last changes fastest.
Arguments:
- grad_embed: bfloat16 [8, 2000, 4608], P('dp')
- grad_q: bfloat16 [8, 6, 4608, 32], P('dp')
- grad_k: bfloat16 [8, 6, 4608, 16], P('dp')
- grad_v: bfloat16 [8, 6, 4608, 16], P('dp')
- grad_out: bfloat16 [8, 6, 32, 4608], P('dp')
- grad_gate: bfloat16 [8, 6, 4608, 288], P('dp')
- grad_up: bfloat16 [8, 6, 4608, 288], P('dp')
- grad_down: bfloat16 [8, 6, 288, 4608], P('dp')
- grad_norms: bfloat16 [8, 6, 4, 4608], P('dp')
- grad_qk_norms: bfloat16 [8, 6, 2, 128], P('dp')
- first_moment: float32 [35870208], P('dp')
- second_moment: float32 [35870208], P('dp')
- master_param: float32 [35870208], P('dp')
- hyper_params: float32 [5], replicated
Outputs:
- output 1: bfloat16 [2000, 4608], replicated
- output 2: bfloat16 [6, 4608, 32], replicated
- output 3: bfloat16 [6, 4608, 16], replicated
- output 4: bfloat16 [6, 4608, 16], replicated
- output 5: bfloat16 [6, 32, 4608], replicated
- output 6: bfloat16 [6, 4608, 288], replicated
- output 7: bfloat16 [6, 4608, 288], replicated
- output 8: bfloat16 [6, 288, 4608], replicated
- output 9: bfloat16 [6, 4, 4608], replicated
- output 10: bfloat16 [6, 2, 128], replicated
- output 11: float32 [35870208], P('dp')
- output 12: float32 [35870208], P('dp')
- output 13: float32 [35870208], P('dp')
All inputs are finite; a program needn't handle non-finite values.
Results may differ from the reference program's by a relative error of at most 0.001.
Values are sent between devices in bfloat16 or wider.
A program may use at most 1 GiB of HBM per device.

```python
import math
import jax
import jax.numpy as jnp

D_MODEL = 4608
FF_WIDTH = 36864
Q_HEADS = 32
KV_HEADS = 16
HEAD_DIM = 128
VOCAB_SIZE = 256000
TP_RANKS = 128
NUM_LAYERS = 6
DATA_PAR = 8
ADAM_STEP = 7

ADAM_EPS = 1e-8
CLIP_EPS = 1e-6
Q_COLS = Q_HEADS * HEAD_DIM // TP_RANKS
KV_COLS = KV_HEADS * HEAD_DIM // TP_RANKS
FF_COLS = FF_WIDTH // TP_RANKS
VOCAB_ROWS = VOCAB_SIZE // TP_RANKS
PARAM_SHAPES = ((VOCAB_ROWS, D_MODEL), (NUM_LAYERS, D_MODEL, Q_COLS), (NUM_LAYERS, D_MODEL, KV_COLS), (NUM_LAYERS, D_MODEL, KV_COLS), (NUM_LAYERS, Q_COLS, D_MODEL), (NUM_LAYERS, D_MODEL, FF_COLS), (NUM_LAYERS, D_MODEL, FF_COLS), (NUM_LAYERS, FF_COLS, D_MODEL), (NUM_LAYERS, 4, D_MODEL), (NUM_LAYERS, 2, HEAD_DIM))
PARAM_SIZES = tuple(math.prod(tensor_dims) for tensor_dims in PARAM_SHAPES)
PARAMS_TOTAL = sum(PARAM_SIZES)
DECAY_LEN = PARAMS_TOTAL - PARAM_SIZES[8] - PARAM_SIZES[9]
GRAD_NAMES = ("grad_embed", "grad_q", "grad_k", "grad_v", "grad_out", "grad_gate", "grad_up", "grad_down", "grad_norms", "grad_qk_norms")


def setup_inputs(seed: int = 0) -> dict:
    key_list = jax.random.split(jax.random.key(seed), 16)
    grad_scale = math.sqrt(DATA_PAR)
    inputs = {}
    square_sum = jnp.float32(0.0)
    for tensor_index, tensor_dims in enumerate(PARAM_SHAPES):
        noise_draw = jax.random.normal(key_list[tensor_index], (DATA_PAR,) + tensor_dims, jnp.float32)
        grad_arr = (grad_scale * noise_draw).astype(jnp.bfloat16)
        mean_grad = jnp.sum(grad_arr, axis=0, dtype=jnp.float32) / DATA_PAR
        square_sum = square_sum + jnp.sum(mean_grad * mean_grad)
        inputs[GRAD_NAMES[tensor_index]] = grad_arr
    inputs["first_moment"] = 0.1 * jax.random.normal(key_list[10], (PARAMS_TOTAL,), jnp.float32)
    inputs["second_moment"] = 0.015 * jnp.exp(0.5 * jax.random.normal(key_list[11], (PARAMS_TOTAL,), jnp.float32))
    inputs["master_param"] = 0.5 * jax.random.normal(key_list[12], (PARAMS_TOTAL,), jnp.float32)
    hyper_draw = jax.random.uniform(key_list[13], (5,), jnp.float32)
    inputs["hyper_params"] = jnp.stack([0.05 + 0.1 * hyper_draw[0], 0.8 + 0.15 * hyper_draw[1], 0.9 + 0.09 * hyper_draw[2], 0.3 + 1.2 * hyper_draw[3], (0.3 + 0.4 * hyper_draw[4]) * jnp.sqrt(square_sum)])
    return inputs


def reference(grad_embed, grad_q, grad_k, grad_v, grad_out, grad_gate, grad_up, grad_down, grad_norms, grad_qk_norms, first_moment, second_moment, master_param, hyper_params):
    grads = (grad_embed, grad_q, grad_k, grad_v, grad_out, grad_gate, grad_up, grad_down, grad_norms, grad_qk_norms)
    mean_grad = jnp.concatenate([jnp.sum(grad_arr, axis=0, dtype=jnp.float32).reshape(-1) for grad_arr in grads]) / DATA_PAR
    learn_rate = hyper_params[0]
    beta_one = hyper_params[1]
    beta_two = hyper_params[2]
    weight_decay = hyper_params[3]
    grad_norm = jnp.sqrt(jnp.sum(mean_grad * mean_grad))
    clip_scale = jnp.minimum(1.0, hyper_params[4] / (grad_norm + CLIP_EPS))
    clipped = mean_grad * clip_scale
    moment_one = beta_one * first_moment + (1.0 - beta_one) * clipped
    moment_two = beta_two * second_moment + (1.0 - beta_two) * (clipped * clipped)
    m_hat = moment_one / (1.0 - beta_one ** ADAM_STEP)
    v_hat = moment_two / (1.0 - beta_two ** ADAM_STEP)
    keep_decay = jnp.arange(PARAMS_TOTAL) < DECAY_LEN
    direction = m_hat / (jnp.sqrt(v_hat) + ADAM_EPS) + jnp.where(keep_decay, weight_decay * master_param, 0.0)
    new_master = master_param - learn_rate * direction
    new_params = new_master.astype(jnp.bfloat16)
    out_list = []
    start_pos = 0
    for tensor_dims, tensor_size in zip(PARAM_SHAPES, PARAM_SIZES):
        out_list.append(new_params[start_pos:start_pos + tensor_size].reshape(tensor_dims))
        start_pos = start_pos + tensor_size
    return (out_list[0], out_list[1], out_list[2], out_list[3], out_list[4], out_list[5], out_list[6], out_list[7], out_list[8], out_list[9], moment_one, moment_two, new_master)
```

```python
import functools
import math
import jax
import jax.numpy as jnp
from jax import lax
from jax.experimental import pallas as pl
from jax.experimental.pallas import tpu as pltpu
from jax.sharding import PartitionSpec as P

ADAM_STEP = 7
ADAM_EPS = 1e-8
CLIP_EPS = 1e-6
GRAD_COUNT = 10
NORM_COUNT = 2
MESH = pl.DeviceIdType.MESH

GROUP = 8
HALVES = range(2)
OTHERS = range(1, GROUP)
BLK = 36864
ROWS = 288
SHARE = 4483776
HALF = 62
COVER = 2 * HALF
CH = 2
CHUNKS = HALF // CH
AHEAD = 3
SLOTS = 8
OWN = 122
OWN_HALF = OWN // 2
EDGES = (0, 250, 274, 286, 298, 322, 538, 754, 970, 974)
TAIL_BLOCKS = 6
TILE = (36, 8, 128)
COLS = 36
GATHER_CHUNKS = (8, 8, 8, 8, 8, 8, 8, 5)
DECAY_LEN = 970 * BLK


def cover_start(r):
    return (r * SHARE) // BLK


def own_start(r):
    return (r * SHARE + BLK - 1) // BLK


def kind_of(b):
    is_q = (b >= EDGES[1]) & (b < EDGES[2])
    is_kv = (b >= EDGES[2]) & (b < EDGES[4])
    is_gate = (b >= EDGES[5]) & (b < EDGES[7])
    is_row = (b < EDGES[1]) | ((b >= EDGES[4]) & (b < EDGES[5])) | (b >= EDGES[7])
    return is_row, is_gate, is_q, is_kv


def lane_pick(parts, width):
    lane = lax.broadcasted_iota(jnp.int32, parts[0].shape, 1)
    out = parts[0]
    for i in range(1, len(parts)):
        out = jnp.where(lane >= i * width, parts[i], out)
    return out


def roll_to(x, src, dst):
    shift = (dst - src) % 128
    return pltpu.roll(x, shift, 1) if shift else x


def tile_order(kind):
    if kind == "gate":
        return list(range(36))
    if kind == "q":
        return [rt * 9 + ct for ct in range(9) for rt in range(4)]
    return [rt * 18 + ct for ct in range(18) for rt in HALVES]


def pieces(kind):
    out = []
    if kind == "gate":
        for f in range(9):
            for q in range(4):
                k = 4 * f + q
                dd, a = k // 9, k % 9
                out.append(((f, 32, 9), q, (a // 4, dd, 4), a % 4))
    elif kind == "q":
        for ct in range(9):
            for q in range(4):
                out.append(((32 * ct, 32, 1), q, (ct // 4, q, 4), ct % 4))
    else:
        for ct in range(18):
            for q in range(8):
                out.append(((16 * ct, 16, 1), q, (ct // 8, q, 8), ct % 8))
    return out


def width_of(kind):
    return 16 if kind == "kv" else 32


def rows_to_joined(src, dst):
    for i in range(8):
        dst[pl.ds(36 * i, 36), :] = src[:, i, :]


def joined_to_rows(src, emit):
    for t in range(36):
        emit(t, src[pl.ds(t, 8, stride=36), :])


def transposed_to_joined(kind, src, tbuf, dst):
    order = tile_order(kind)
    for j in range(3):
        tiles = [src[t] for t in order[16 * j:16 * j + 16]]
        if len(tiles) < 16:
            tiles.append(jnp.zeros((128 - 8 * len(tiles), 128), jnp.float32))
        tbuf[j] = jnp.concatenate(tiles, axis=0).T
    w = width_of(kind)
    groups = {}
    for drows, dl, srows, sl in pieces(kind):
        groups.setdefault(drows, []).append((dl, srows, sl))
    for (start, count, stride), items in groups.items():
        parts = [None] * (128 // w)
        for dl, (g, s0, sstr), sl in items:
            parts[dl] = roll_to(tbuf[g, pl.ds(s0, count, stride=sstr), :], sl * w, dl * w)
        value = lane_pick(parts, w)
        if stride == 1:
            dst[pl.ds(start, count), :] = value
        else:
            dst[pl.ds(start, count, stride=stride), :] = value


def joined_to_transposed(kind, src, tbuf, emit):
    order = tile_order(kind)
    w = width_of(kind)
    groups = {}
    for drows, dl, srows, sl in pieces(kind):
        groups.setdefault(srows, []).append((sl, drows, dl))
    for (g, s0, sstr), items in groups.items():
        count = items[0][1][1]
        parts = [None] * (128 // w)
        for sl, (start, cnt, stride), dl in items:
            if stride == 1:
                rows = src[pl.ds(start, cnt), :]
            else:
                rows = src[pl.ds(start, cnt, stride=stride), :]
            parts[sl] = roll_to(rows, dl * w, sl * w)
        filler = next(p for p in parts if p is not None)
        parts = [filler if p is None else p for p in parts]
        tbuf[g, pl.ds(s0, count, stride=sstr), :] = lane_pick(parts, w)
    for j in range(3):
        block = tbuf[j].T
        for n, t in enumerate(order[16 * j:16 * j + 16]):
            emit(t, block[8 * n:8 * n + 8, :])


def positions(me):
    y, x, c = me // 4, (me // 2) % 2, me % 2
    xn, yn = 1 - x, 1 - y
    return y, x, c, xn, yn


def dev(y, x, c):
    return (y * 2 + x) * 2 + c


def by_block(b, refs, fn):
    embed, small, gate, up, down, tail = refs
    e = EDGES

    def span(lo, hi, view):
        @pl.when((b >= lo) & (b < hi))
        def _():
            fn(view(b - lo))
    span(0, e[1], lambda n: embed.at[n])
    span(e[1], e[5], lambda n: small.at[n])
    span(e[5], e[6], lambda n: gate.at[n // COLS, :, n % COLS])
    span(e[6], e[7], lambda n: up.at[n // COLS, :, n % COLS])
    span(e[7], e[8], lambda n: down.at[n])
    span(e[8], e[8] + TAIL_BLOCKS, lambda n: tail.at[n])


def reduce_kernel(e_in, q_in, gate_in, up_in, down_in, tail_in, g_hbm, nrm_ref, r1, r2, ld, ld2, st, sbuf, tbuf, fbuf, acc, nbuf,
                  s1_send, s1_recv, s2_send, s2_recv, ld_sem, g_sem, n_send, n_recv):
    me = lax.axis_index("dp")
    y, x, c, xn, yn = positions(me)
    sources = (e_in, q_in, gate_in, up_in, down_in, tail_in)
    barrier = pltpu.get_barrier_semaphore()
    for o in OTHERS:
        pl.semaphore_signal(barrier, inc=1, device_id=((me + o) % GROUP,), device_id_type=MESH)
    pl.semaphore_wait(barrier, GROUP - 1)

    partner = dev(y, x, 1 - c)
    def targets(h):
        cy, cx = (y, xn) if h == 0 else (yn, x)
        oy, ox = (1 - cy, cx) if h == 0 else (cy, 1 - cx)
        py, px = (1 - y, x) if h == 0 else (y, 1 - x)
        return (
            (partner, 0, (dev(py, px, 1 - c), partner)),
            (dev(cy, cx, 0), 1 + c, (dev(oy, ox, 0), dev(cy, cx, 0))),
            (dev(cy, cx, 1), 1 + c, (dev(oy, ox, 1), dev(cy, cx, 1))),
        )

    def send(h, n, t):
        d, k = t // CHUNKS, t % CHUNKS
        device, slot, dests = targets(h)[n]
        dest = dests[0] * (1 - d) + dests[1] * d
        for j in range(CH):
            at = k * CH + j

            def start(src):
                pltpu.make_async_remote_copy(
                    src_ref=src, dst_ref=r1.at[h, slot, d, at],
                    send_sem=s1_send.at[h, n, t % SLOTS], recv_sem=s1_recv.at[h, slot, t],
                    device_id=(device,), device_id_type=MESH).start()
            by_block(cover_start(dest) + h * HALF + at, sources, start)

    def sent(h, n, t):
        view = ld.at[h, 0]
        pltpu.make_async_copy(view, view, s1_send.at[h, n, t % SLOTS]).wait()

    total_steps = 2 * CHUNKS

    def issue(t):
        @pl.when(t < total_steps)
        def _():
            for n in (1, 2, 0):
                for h in HALVES:
                    @pl.when(t >= SLOTS)
                    def _():
                        sent(h, n, t - SLOTS)
                    send(h, n, t)

    def first_issue(t, carry):
        issue(t)
        return carry

    lax.fori_loop(0, AHEAD, first_issue, 0)

    other = (dev(yn, x, c), dev(y, xn, c))

    def wait_stage1(h, t):
        d, k = t // CHUNKS, t % CHUNKS
        for slot in range(3):
            view = r1.at[h, slot, d, pl.ds(k * CH, CH)]
            pltpu.make_async_copy(view, view, s1_recv.at[h, slot, t]).wait()

    def start_loads(h, t, dest):
        d, k = t // CHUNKS, t % CHUNKS
        for j in range(CH):
            def start(src):
                pltpu.make_async_copy(src, ld.at[h, 3, j], ld_sem.at[h, 3]).start()
            by_block(cover_start(dest) + h * HALF + k * CH + j, sources, start)
        for slot in range(3):
            pltpu.make_async_copy(
                r1.at[h, slot, d, pl.ds(k * CH, CH)], ld.at[h, slot], ld_sem.at[h, slot]).start()

    def wait_loads(h):
        for slot in range(4):
            pltpu.make_async_copy(ld.at[h, slot], ld.at[h, slot], ld_sem.at[h, slot]).wait()

    def partial_sum(h, j, t0):
        rows = [ld[h, s, j, pl.ds(t0, 4)].astype(jnp.float32) for s in range(4)]
        return (rows[3] + rows[0]) + (rows[1] + rows[2])

    def stage2_copy(h, k):
        return pltpu.make_async_remote_copy(
            src_ref=st.at[h, k % SLOTS], dst_ref=r2.at[h, pl.ds(k * CH, CH)],
            send_sem=s2_send.at[h, k % SLOTS], recv_sem=s2_recv.at[h, k],
            device_id=(other[h],), device_id_type=MESH)

    def other_step(k, carry):
        issue(k + AHEAD)
        for h in HALVES:
            wait_stage1(h, k)
            start_loads(h, k, other[h])
        for h in HALVES:
            @pl.when(k >= SLOTS)
            def _():
                stage2_copy(h, k - SLOTS).wait_send()
            wait_loads(h)
            for j in range(CH):
                def add(i, z):
                    st[h, k % SLOTS, j, pl.ds(i * 4, 4)] = partial_sum(h, j, i * 4)
                    return z
                lax.fori_loop(0, 9, add, 0)
            stage2_copy(h, k).start()
        return carry

    lax.fori_loop(0, CHUNKS, other_step, 0)

    acc[...] = jnp.zeros_like(acc)
    first, last = own_start(me), own_start(me + 1)

    def g_copy(h, k):
        row = pl.multiple_of((h * HALF + k * CH) * ROWS, 8)
        return pltpu.make_async_copy(
            fbuf.at[h, k % 2], g_hbm.at[pl.ds(row, CH * ROWS)], g_sem.at[h, k % 2])

    def own_step(k, carry):
        t = k + CHUNKS
        issue(t + AHEAD)
        for h in HALVES:
            wait_stage1(h, t)
            view = r2.at[h, pl.ds(k * CH, CH)]
            pltpu.make_async_copy(view, view, s2_recv.at[h, k]).wait()
            start_loads(h, t, me)
            pltpu.make_async_copy(view, ld2.at[h], ld_sem.at[h, 4]).start()
        for h in HALVES:
            @pl.when(k >= 2)
            def _():
                g_copy(h, k - 2).wait()
            wait_loads(h)
            pltpu.make_async_copy(ld2.at[h], ld2.at[h], ld_sem.at[h, 4]).wait()
            for j in range(CH):
                b = cover_start(me) + h * HALF + k * CH + j
                weight = jnp.where((b >= first) & (b < last), 1.0, 0.0)

                def add(i, z):
                    s = partial_sum(h, j, i * 4) + ld2[h, j, pl.ds(i * 4, 4)]
                    sbuf[pl.ds(i * 4, 4)] = s
                    return z + jnp.sum(s * s, axis=0)
                sq = lax.fori_loop(0, 9, add, jnp.zeros((8, 128), jnp.float32))
                acc[...] += sq * weight
                dst = fbuf.at[h, k % 2, pl.ds(j * ROWS, ROWS)]
                is_row, is_gate, is_q, is_kv = kind_of(b)
                pl.when(is_row)(functools.partial(rows_to_joined, sbuf, dst))
                pl.when(is_gate)(functools.partial(transposed_to_joined, "gate", sbuf, tbuf, dst))
                pl.when(is_q)(functools.partial(transposed_to_joined, "q", sbuf, tbuf, dst))
                pl.when(is_kv)(functools.partial(transposed_to_joined, "kv", sbuf, tbuf, dst))
            g_copy(h, k).start()
        return carry

    lax.fori_loop(0, CHUNKS, own_step, 0)

    nbuf[me] = acc[...]

    def norm_copy(o):
        return pltpu.make_async_remote_copy(
            src_ref=acc, dst_ref=nbuf.at[me], send_sem=n_send.at[o - 1], recv_sem=n_recv.at[me],
            device_id=((me + o) % GROUP,), device_id_type=MESH)

    for o in OTHERS:
        norm_copy(o).start()
    for h in HALVES:
        for k in range(CHUNKS - 2, CHUNKS):
            g_copy(h, k).wait()
        for k in range(CHUNKS - SLOTS, CHUNKS):
            stage2_copy(h, k).wait_send()
        for n in range(3):
            for t in range(total_steps - SLOTS, total_steps):
                sent(h, n, t)
    for o in OTHERS:
        peer = (me + o) % GROUP
        pltpu.make_async_copy(nbuf.at[peer], nbuf.at[peer], n_recv.at[peer]).wait()
    for o in OTHERS:
        norm_copy(o).wait_send()
    total = nbuf[0]
    for i in OTHERS:
        total = total + nbuf[i]
    nrm_ref[...] = total


def run_reduce(sources):
    any_spec = pl.BlockSpec(memory_space=pl.ANY)
    f32, bf16 = jnp.float32, jnp.bfloat16
    tile = TILE
    out_shape = (
        jax.ShapeDtypeStruct((COVER * ROWS, 128), f32),
        jax.ShapeDtypeStruct((8, 128), f32),
        jax.ShapeDtypeStruct((2, 3, 2, HALF) + tile, bf16),
        jax.ShapeDtypeStruct((2, HALF) + tile, f32),
    )
    dma = pltpu.SemaphoreType.DMA
    outs = pl.pallas_call(
        reduce_kernel, out_shape=out_shape, in_specs=[any_spec] * len(sources),
        out_specs=(any_spec, pl.BlockSpec(memory_space=pltpu.VMEM), any_spec, any_spec),
        scratch_shapes=[
            pltpu.VMEM((2, 4, CH) + tile, bf16),
            pltpu.VMEM((2, CH) + tile, f32),
            pltpu.VMEM((2, SLOTS, CH) + tile, f32),
            pltpu.VMEM(tile, f32),
            pltpu.VMEM((3, 128, 128), f32),
            pltpu.VMEM((2, 2, CH * ROWS, 128), f32),
            pltpu.VMEM((8, 128), f32),
            pltpu.VMEM((GROUP, 8, 128), f32),
            dma((2, 3, SLOTS)), dma((2, 3, 2 * CHUNKS)), dma((2, SLOTS)), dma((2, CHUNKS)),
            dma((2, 5)), dma((2, 2)), dma((GROUP - 1,)), dma((GROUP,)),
        ],
        compiler_params=pltpu.CompilerParams(collective_id=0, has_side_effects=True),
        name="reduce_scatter",
    )(*sources)
    return outs[0], outs[1]


def update_kernel(me_ref, hyper_ref, nrm_ref, g0, g1, m0, v0, p0, mt, vt, pt,
                  m_out, v_out, p_out, o_ref, gbuf, pbuf, fbuf, tbuf, cbuf):
    i = pl.program_id(0)
    me = me_ref[0]
    lr, b1, b2, wd, max_norm = [hyper_ref[n] for n in range(5)]
    delta = me * SHARE - cover_start(me) * BLK
    rho, odd = delta // 128, me % 2 == 1
    low, high = pl.ds(0, ROWS), pl.ds(ROWS, ROWS)

    def place(buf, at, count, x):
        @pl.when(odd)
        def _():
            buf[pl.ds(at, count), :] = pltpu.roll(x(), 64, 1)

        @pl.when(jnp.logical_not(odd))
        def _():
            buf[pl.ds(at, count), :] = x()

    @pl.when(i == 0)
    def _():
        one = jnp.ones((8, 128), jnp.float32)

        def power(b):
            square = b * b
            cube = b * square
            return cube * (square * square)

        norm = jnp.sqrt(jnp.sum(nrm_ref[...], keepdims=True) * (1.0 / 64.0))
        clip = jnp.minimum(1.0, (one * max_norm) / (norm + CLIP_EPS))
        cbuf[0] = clip * 0.125
        cbuf[1] = one / (one * (1.0 - power(b1)))
        cbuf[2] = one / (one * (1.0 - power(b2)))
        place(gbuf, ROWS, ROWS, lambda: g0[...])

    gbuf[low, :] = gbuf[high, :]
    pbuf[low, :] = pbuf[high, :]
    place(gbuf, ROWS, ROWS, lambda: g1[...])
    size = 32
    scale, inv1, inv2 = [cbuf[n, :1] for n in range(3)]
    lane = lax.broadcasted_iota(jnp.int32, (size, 128), 1)
    sub = lax.broadcasted_iota(jnp.int32, (size, 128), 0)
    own_lane = (lane < 64) | jnp.logical_not(odd)

    def window(buf, row, j):
        at = row + size * j
        return jnp.where(own_lane, buf[pl.ds(at, size), :], buf[pl.ds(at + 1, size), :])

    def run(ms, vs, ps, keep):
        for j in range(ROWS // size):
            part = pl.ds(size * 128 * j, size * 128)
            h = window(gbuf, rho, j) * scale
            m, v, p = [r[part].reshape(size, 128) for r in (ms, vs, ps)]
            m1 = b1 * m + (1.0 - b1) * h
            v1 = b2 * v + (1.0 - b2) * (h * h)
            pos = me * SHARE + i * BLK + size * 128 * j + sub * 128 + lane
            decay = jnp.where(pos < DECAY_LEN, wd * p, 0.0)
            u = (m1 * inv1) / (jnp.sqrt(v1 * inv2) + ADAM_EPS) + decay
            p1 = p - lr * u
            place(pbuf, ROWS + size * j, size, lambda: p1)

            @pl.when(keep)
            def _():
                m_out[part] = m1.reshape(size * 128)
                v_out[part] = v1.reshape(size * 128)
                p_out[part] = p1.reshape(size * 128)

    pl.when(i < 121)(lambda: run(m0, v0, p0, True))
    pl.when(i >= 121)(lambda: run(mt, vt, pt, i < OWN))

    @pl.when(i >= 1)
    def _():
        sigma = (own_start(me) * BLK - me * SHARE) // 128
        for j in range(ROWS // size):
            fbuf[pl.ds(size * j, size), :] = window(pbuf, sigma, j)
        b = own_start(me) + i - 1

        def emit(t, value):
            o_ref[0, t] = value.astype(jnp.bfloat16)
        is_row, is_gate, is_q, is_kv = kind_of(b)
        pl.when(is_row)(functools.partial(joined_to_rows, fbuf, emit))
        pl.when(is_gate)(functools.partial(joined_to_transposed, "gate", fbuf, tbuf, emit))
        pl.when(is_q)(functools.partial(joined_to_transposed, "q", fbuf, tbuf, emit))
        pl.when(is_kv)(functools.partial(joined_to_transposed, "kv", fbuf, tbuf, emit))


def run_update(me, hyper, nrm, g, state, tails):
    f32 = jnp.float32
    flat = lambda f: pl.BlockSpec((BLK,), f)
    main = flat(lambda i, me: (jnp.minimum(i, 120),))
    tail = flat(lambda i, me: (jnp.maximum(i - 121, 0),))
    out = flat(lambda i, me: (jnp.minimum(i, 121),))
    return pl.pallas_call(
        update_kernel,
        grid_spec=pltpu.PrefetchScalarGridSpec(
            num_scalar_prefetch=1, grid=(OWN + 1,),
            in_specs=[
                pl.BlockSpec(memory_space=pltpu.SMEM),
                pl.BlockSpec((8, 128), lambda i, me: (0, 0)),
                pl.BlockSpec((ROWS, 128), lambda i, me: (0, 0)),
                pl.BlockSpec((ROWS, 128), lambda i, me: (i + 1, 0)),
                main, main, main, tail, tail, tail],
            out_specs=[out, out, out,
                       pl.BlockSpec((1, 36, 8, 128), lambda i, me: (me[0] * OWN + jnp.maximum(i - 1, 0), 0, 0, 0))],
            scratch_shapes=[
                pltpu.VMEM((2 * ROWS + 8, 128), f32), pltpu.VMEM((2 * ROWS + 8, 128), f32),
                pltpu.VMEM((ROWS, 128), f32), pltpu.VMEM((3, 128, 128), f32),
                pltpu.VMEM((3, 8, 128), f32)]),
        out_shape=[jax.ShapeDtypeStruct((SHARE,), f32)] * 3
        + [jax.ShapeDtypeStruct((GROUP * OWN, 36, 8, 128), jnp.bfloat16)],
        compiler_params=pltpu.CompilerParams(dimension_semantics=("arbitrary",)),
        name="adam_update",
    )(me, hyper, nrm, g, g, *state, *tails)


def gather_kernel(o_in, o, f_send, f_recv, s_send, s_recv, p_send, p_recv):
    me = lax.axis_index("dp")
    y, x, c, xn, yn = positions(me)
    partner = dev(y, x, 1 - c)
    near = (dev(yn, x, c), dev(y, xn, c))
    far = dev(yn, xn, c)
    barrier = pltpu.get_barrier_semaphore()
    for device in (partner, near[0], near[1]):
        pl.semaphore_signal(barrier, inc=1, device_id=(device,), device_id_type=MESH)
    pl.semaphore_wait(barrier, 3)

    starts = [sum(GATHER_CHUNKS[:n]) for n in range(len(GATHER_CHUNKS))]

    def span(h, share, n):
        return o.at[pl.ds(share * OWN + h * OWN_HALF + starts[n], GATHER_CHUNKS[n])]

    def copy(h, share, n, send, recv, device):
        return pltpu.make_async_remote_copy(
            src_ref=span(h, share, n), dst_ref=span(h, share, n), send_sem=send, recv_sem=recv,
            device_id=(device,), device_id_type=MESH)

    def first_hop(h, n):
        return copy(h, me, n, f_send.at[h, n], f_recv.at[h, n], near[h])

    def second_hop(h, which, n):
        share = (me, near[h])[which]
        return copy(h, share, n, s_send.at[h, which, n], s_recv.at[h, which, n], near[1 - h])

    shares = lambda h: (me, near[h], near[1 - h], far)

    def to_partner(h, which, n):
        return copy(h, shares(h)[which], n, p_send.at[h, which, n], p_recv.at[h, which, n], partner)

    def arrived(h, share, n, sem):
        pltpu.make_async_copy(span(h, share, n), span(h, share, n), sem).wait()

    count = len(GATHER_CHUNKS)
    for n in range(count):
        for h in HALVES:
            first_hop(h, n).start()
            second_hop(h, 0, n).start()
    for n in range(count):
        for h in HALVES:
            to_partner(h, 0, n).start()
    for n in range(count):
        for h in HALVES:
            arrived(h, near[h], n, f_recv.at[h, n])
            second_hop(h, 1, n).start()
            to_partner(h, 1, n).start()
        for h in HALVES:
            arrived(h, near[1 - h], n, s_recv.at[h, 0, n])
            to_partner(h, 2, n).start()
    for n in range(count):
        for h in HALVES:
            arrived(h, far, n, s_recv.at[h, 1, n])
            to_partner(h, 3, n).start()
    ps = dev(y, x, 1 - c)
    pshares = lambda h: (ps, (dev(yn, x, 1 - c), dev(y, xn, 1 - c))[h],
                         (dev(yn, x, 1 - c), dev(y, xn, 1 - c))[1 - h], dev(yn, xn, 1 - c))
    for which in range(4):
        for n in range(count):
            for h in HALVES:
                arrived(h, pshares(h)[which], n, p_recv.at[h, which, n])
                to_partner(h, which, n).wait_send()
    for n in range(count):
        for h in HALVES:
            first_hop(h, n).wait_send()
            for which in HALVES:
                second_hop(h, which, n).wait_send()


def run_gather(o):
    any_spec = pl.BlockSpec(memory_space=pl.ANY)
    dma = pltpu.SemaphoreType.DMA
    count = len(GATHER_CHUNKS)
    return pl.pallas_call(
        gather_kernel, out_shape=jax.ShapeDtypeStruct(o.shape, o.dtype),
        in_specs=[any_spec], out_specs=any_spec, input_output_aliases={0: 0},
        scratch_shapes=[dma((2, count)), dma((2, count)), dma((2, 2, count)), dma((2, 2, count)),
                        dma((2, 4, count)), dma((2, 4, count))],
        compiler_params=pltpu.CompilerParams(collective_id=1, has_side_effects=True),
        name="all_gather",
    )(o)


def pack(grads):
    embed, q, k, v, out, gate, up, down, norms, qk = [g[0] for g in grads]

    def rows(a):
        return a.reshape(-1, 8, COLS, 128).transpose(0, 2, 1, 3)

    def grid(a):
        layers, wide, high = a.shape
        return a.transpose(0, 2, 1).reshape(layers, high // 8, 8, COLS, 128).transpose(0, 1, 3, 2, 4)

    def cols(a, parts):
        a = grid(a)
        a = a.reshape(a.shape[0], a.shape[1], parts, -1, 8, 128).swapaxes(1, 2)
        return a.reshape((-1,) + TILE)

    tail = jnp.concatenate([norms.reshape(-1), qk.reshape(-1)])
    tail = jnp.pad(tail, (0, TAIL_BLOCKS * BLK - tail.shape[0]))
    small = jnp.concatenate([cols(q, 4), cols(k, 2), cols(v, 2), rows(out)])
    return rows(embed), small, grid(gate), grid(up), rows(down), rows(tail.reshape(-1, 4608))


def block_runs(b0, b1):
    cuts = [own_start(r) for r in range(GROUP + 1)]
    out = []
    for r in range(GROUP):
        lo, hi = max(b0, cuts[r]), min(b1, cuts[r + 1])
        if lo < hi:
            out.append((r * OWN + lo - cuts[r], hi - lo))
    return out


def unpack_kernel(o, embed, q, k, v, out, gate, up, down, tail, buf, in_sem, out_sem):
    def rows_out(ref, first):
        def store(slot, count):
            pltpu.make_async_copy(
                buf.at[slot, pl.ds(0, count)], ref.at[pl.ds(first, count)], out_sem.at[slot]).start()
        return store

    def grid_out(ref, layer):
        def store(slot, count):
            def one(rt, z):
                pltpu.make_async_copy(buf.at[slot, :, rt], ref.at[layer, rt], out_sem.at[slot]).start()
                return z
            lax.fori_loop(0, COLS, one, 0)
        return store

    def cols_out(ref, parts):
        high, wide = ref.shape[1], COLS // parts

        def store(slot, count):
            def one(n, z):
                for rt in range(high):
                    pltpu.make_async_copy(
                        buf.at[slot, n, pl.ds(wide * rt, wide)],
                        ref.at[n // parts, rt, pl.ds((n % parts) * wide, wide)], out_sem.at[slot]).start()
                return z
            lax.fori_loop(0, count, one, 0)
        return store

    jobs = []

    def add_rows(ref, b0, b1):
        for lo in range(b0, b1, COLS):
            hi = min(lo + COLS, b1)
            jobs.append((lo, hi - lo, rows_out(ref, lo - b0)))

    e = EDGES
    add_rows(embed, e[0], e[1])
    for layer in range(gate.shape[0]):
        jobs.append((e[5] + COLS * layer, COLS, grid_out(gate, layer)))
        jobs.append((e[6] + COLS * layer, COLS, grid_out(up, layer)))
    jobs.append((e[1], e[2] - e[1], cols_out(q, 4)))
    jobs.append((e[2], e[3] - e[2], cols_out(k, 2)))
    jobs.append((e[3], e[4] - e[3], cols_out(v, 2)))
    add_rows(out, e[4], e[5])
    add_rows(down, e[7], e[8])
    add_rows(tail, e[8], e[9])
    depth = buf.shape[0]

    def load(n):
        b0, count, _ = jobs[n]
        at = 0
        for first, size in block_runs(b0, b0 + count):
            pltpu.make_async_copy(
                o.at[pl.ds(first, size)], buf.at[n % depth, pl.ds(at, size)], in_sem.at[n % depth]).start()
            at += size

    def wait(n, sem):
        view = buf.at[n % depth, pl.ds(0, jobs[n][1])]
        pltpu.make_async_copy(view, view, sem.at[n % depth]).wait()

    lead = depth // 2
    for n in range(len(jobs) + lead):
        if n < len(jobs):
            if n >= depth:
                wait(n - depth, out_sem)
            load(n)
        if n >= lead:
            wait(n - lead, in_sem)
            jobs[n - lead][2]((n - lead) % depth, jobs[n - lead][1])
    for n in range(len(jobs) - depth, len(jobs)):
        wait(n, out_sem)


def run_unpack(o, shapes):
    e, bf16 = EDGES, jnp.bfloat16
    any_spec = pl.BlockSpec(memory_space=pl.ANY)

    def rows(n):
        return (n,) + TILE

    def grid(shape):
        return (shape[0], shape[2] // 8) + TILE
    views = [rows(e[1]), grid(shapes[1]), grid(shapes[2]), grid(shapes[3]), rows(e[5] - e[4]),
             grid(shapes[5]), grid(shapes[6]), rows(e[8] - e[7]), rows(e[9] - e[8])]
    dma = pltpu.SemaphoreType.DMA
    depth = 6
    outs = pl.pallas_call(
        unpack_kernel, out_shape=[jax.ShapeDtypeStruct(s, bf16) for s in views],
        in_specs=[any_spec], out_specs=[any_spec] * len(views),
        scratch_shapes=[pltpu.VMEM((depth, COLS) + TILE, bf16), dma((depth,)), dma((depth,))],
        name="unpack",
    )(o)

    def from_rows(a, shape):
        return a.swapaxes(1, 2).reshape(shape)

    def from_grid(a, shape):
        layers, wide, high = shape
        return a.swapaxes(2, 3).reshape(layers, high, wide).swapaxes(1, 2)
    params = [(from_grid if len(a.shape) > 4 else from_rows)(a, s) for a, s in zip(outs[:8], shapes)]
    tail = from_rows(outs[8], (-1,))
    size = math.prod(shapes[8])
    params.append(tail[:size].reshape(shapes[8]))
    params.append(tail[size:size + math.prod(shapes[9])].reshape(shapes[9]))
    return tuple(params)


def solution(mesh):
    group_size = mesh.shape["dp"]
    assert group_size == GROUP

    def local_update(*arrays):
        grads = arrays[:GRAD_COUNT]
        first_part, second_part, master_part, hyper_params = arrays[GRAD_COUNT:]
        state = (first_part, second_part, master_part)
        shapes = [grad_arr.shape[1:] for grad_arr in grads]
        me = lax.axis_index("dp").astype(jnp.int32).reshape(1)

        heads = jnp.concatenate([s[:BLK] for s in state])
        heads = lax.ppermute(heads, "dp", [(r + 1, r) for r in range(GROUP - 1)])
        rest = 2 * BLK - (SHARE - 121 * BLK) - BLK
        tails = [jnp.concatenate([s[121 * BLK:], heads[n * BLK:(n + 1) * BLK], jnp.zeros((rest,), s.dtype)])
                 for n, s in enumerate(state)]

        g, nrm = run_reduce(pack(grads))
        m1, v1, p1, o = run_update(me, hyper_params, nrm, g, state, tails)
        params = run_unpack(run_gather(o), shapes)
        return params + (m1, v1, p1)

    in_specs = tuple([P("dp")] * GRAD_COUNT + [P("dp"), P("dp"), P("dp"), P()])
    out_specs = tuple([P()] * GRAD_COUNT + [P("dp"), P("dp"), P("dp")])
    return jax.shard_map(local_update, mesh=mesh, in_specs=in_specs, out_specs=out_specs, check_vma=False)
```

```python
import functools
import math
import jax
import jax.numpy as jnp
from jax import lax
from jax.experimental import pallas as pl
from jax.experimental.pallas import tpu as pltpu
from jax.sharding import PartitionSpec as P

ADAM_STEP = 7
ADAM_EPS = 1e-8
CLIP_EPS = 1e-6
GRAD_COUNT = 10
NORM_COUNT = 2
MESH = pl.DeviceIdType.MESH

GROUP = 8
PAIR = 2
HALVES = range(PAIR)
OTHERS = range(1, GROUP)
STATE = range(3)
ALL = range(4)
BLK = 36864
ROWS = 288
SHARE = 4483776
HALF = 62
COVER = 2 * HALF
CH = 2
CHUNKS = HALF // CH
AHEAD = 3
SLOTS = 8
OWN = 122
OWN_HALF = OWN // 2
EDGES = (0, 250, 274, 286, 298, 322, 538, 754, 970, 974)
TAIL_BLOCKS = 6
TILE = (36, 8, 128)
COLS = 36
NEAR_LAG = 2
FAR_LAG = 4
DECAY_LEN = 970 * BLK


def cover_start(r):
    return (r * SHARE) // BLK


def own_start(r):
    return (r * SHARE + BLK - 1) // BLK


def kind_of(b):
    is_q = (b >= EDGES[1]) & (b < EDGES[2])
    is_kv = (b >= EDGES[2]) & (b < EDGES[4])
    is_gate = (b >= EDGES[5]) & (b < EDGES[7])
    is_row = (b < EDGES[1]) | ((b >= EDGES[4]) & (b < EDGES[5])) | (b >= EDGES[7])
    return is_row, is_gate, is_q, is_kv


def lane_pick(parts, width):
    lane = lax.broadcasted_iota(jnp.int32, parts[0].shape, 1)
    out = parts[0]
    for i in range(1, len(parts)):
        out = jnp.where(lane >= i * width, parts[i], out)
    return out


def roll_to(x, src, dst):
    shift = (dst - src) % 128
    return pltpu.roll(x, shift, 1) if shift else x


def tile_order(kind):
    if kind == "gate":
        return list(range(36))
    if kind == "q":
        return [rt * 9 + ct for ct in range(9) for rt in range(4)]
    return [rt * 18 + ct for ct in range(18) for rt in HALVES]


def pieces(kind):
    out = []
    if kind == "gate":
        for f in range(9):
            for q in range(4):
                k = 4 * f + q
                dd, a = k // 9, k % 9
                out.append(((f, 32, 9), q, (a // 4, dd, 4), a % 4))
    elif kind == "q":
        for ct in range(9):
            for q in range(4):
                out.append(((32 * ct, 32, 1), q, (ct // 4, q, 4), ct % 4))
    else:
        for ct in range(18):
            for q in range(8):
                out.append(((16 * ct, 16, 1), q, (ct // 8, q, 8), ct % 8))
    return out


def width_of(kind):
    return 16 if kind == "kv" else 32


def rows_to_joined(src, dst):
    for i in range(8):
        dst[pl.ds(36 * i, 36), :] = src[:, i, :]


def joined_to_rows(src, emit):
    for t in range(36):
        emit(t, src[pl.ds(t, 8, stride=36), :])


def transposed_to_joined(kind, src, tbuf, dst):
    order = tile_order(kind)
    for j in range(3):
        tiles = [src[t] for t in order[16 * j:16 * j + 16]]
        if len(tiles) < 16:
            tiles.append(jnp.zeros((128 - 8 * len(tiles), 128), jnp.float32))
        tbuf[j] = jnp.concatenate(tiles, axis=0).T
    w = width_of(kind)
    groups = {}
    for drows, dl, srows, sl in pieces(kind):
        groups.setdefault(drows, []).append((dl, srows, sl))
    for (start, count, stride), items in groups.items():
        parts = [None] * (128 // w)
        for dl, (g, s0, sstr), sl in items:
            parts[dl] = roll_to(tbuf[g, pl.ds(s0, count, stride=sstr), :], sl * w, dl * w)
        value = lane_pick(parts, w)
        if stride == 1:
            dst[pl.ds(start, count), :] = value
        else:
            dst[pl.ds(start, count, stride=stride), :] = value


def joined_to_transposed(kind, src, tbuf, emit):
    order = tile_order(kind)
    w = width_of(kind)
    groups = {}
    for drows, dl, srows, sl in pieces(kind):
        groups.setdefault(srows, []).append((sl, drows, dl))
    for (g, s0, sstr), items in groups.items():
        count = items[0][1][1]
        parts = [None] * (128 // w)
        for sl, (start, cnt, stride), dl in items:
            if stride == 1:
                rows = src[pl.ds(start, cnt), :]
            else:
                rows = src[pl.ds(start, cnt, stride=stride), :]
            parts[sl] = roll_to(rows, dl * w, sl * w)
        filler = next(p for p in parts if p is not None)
        parts = [filler if p is None else p for p in parts]
        tbuf[g, pl.ds(s0, count, stride=sstr), :] = lane_pick(parts, w)
    for j in range(3):
        block = tbuf[j].T
        for n, t in enumerate(order[16 * j:16 * j + 16]):
            emit(t, block[8 * n:8 * n + 8, :])


def positions(me):
    y, x, c = me // 4, (me // 2) % 2, me % 2
    xn, yn = 1 - x, 1 - y
    return y, x, c, xn, yn


def dev(y, x, c):
    return (y * 2 + x) * 2 + c


def by_block(b, refs, fn):
    embed, small, gate, up, down, tail = refs
    e = EDGES

    def span(lo, hi, view):
        @pl.when((b >= lo) & (b < hi))
        def _():
            fn(view(b - lo))
    span(0, e[1], lambda n: embed.at[n])
    span(e[1], e[5], lambda n: small.at[n])
    span(e[5], e[6], lambda n: gate.at[n // COLS, :, n % COLS])
    span(e[6], e[7], lambda n: up.at[n // COLS, :, n % COLS])
    span(e[7], e[8], lambda n: down.at[n])
    span(e[8], e[8] + TAIL_BLOCKS, lambda n: tail.at[n])


def reduce_kernel(e_in, q_in, gate_in, up_in, down_in, tail_in, g_hbm, nrm_ref, r1, r2, ld, ld2, st, sbuf, tbuf, fbuf, acc, nbuf,
                  s1_send, s1_recv, s2_send, s2_recv, ld_sem, g_sem, n_send, n_recv):
    me = lax.axis_index("dp")
    y, x, c, xn, yn = positions(me)
    sources = (e_in, q_in, gate_in, up_in, down_in, tail_in)
    barrier = pltpu.get_barrier_semaphore()
    for o in OTHERS:
        pl.semaphore_signal(barrier, inc=1, device_id=((me + o) % GROUP,), device_id_type=MESH)
    pl.semaphore_wait(barrier, GROUP - 1)

    partner = dev(y, x, 1 - c)
    def targets(h):
        cy, cx = (y, xn) if h == 0 else (yn, x)
        oy, ox = (1 - cy, cx) if h == 0 else (cy, 1 - cx)
        py, px = (1 - y, x) if h == 0 else (y, 1 - x)
        return (
            (partner, 0, (dev(py, px, 1 - c), partner)),
            (dev(cy, cx, 0), 1 + c, (dev(oy, ox, 0), dev(cy, cx, 0))),
            (dev(cy, cx, 1), 1 + c, (dev(oy, ox, 1), dev(cy, cx, 1))),
        )

    def send(h, n, t):
        d, k = t // CHUNKS, t % CHUNKS
        device, slot, dests = targets(h)[n]
        dest = dests[0] * (1 - d) + dests[1] * d
        for j in range(CH):
            at = k * CH + j

            def start(src):
                pltpu.make_async_remote_copy(
                    src_ref=src, dst_ref=r1.at[h, slot, d, at],
                    send_sem=s1_send.at[h, n, t % SLOTS], recv_sem=s1_recv.at[h, slot, t],
                    device_id=(device,), device_id_type=MESH).start()
            by_block(cover_start(dest) + h * HALF + at, sources, start)

    def sent(h, n, t):
        view = ld.at[h, 0]
        pltpu.make_async_copy(view, view, s1_send.at[h, n, t % SLOTS]).wait()

    total_steps = 2 * CHUNKS

    def issue(t):
        @pl.when(t < total_steps)
        def _():
            for n in (1, 2, 0):
                for h in HALVES:
                    @pl.when(t >= SLOTS)
                    def _():
                        sent(h, n, t - SLOTS)
                    send(h, n, t)

    def first_issue(t, carry):
        issue(t)
        return carry

    lax.fori_loop(0, AHEAD, first_issue, 0)

    other = (dev(yn, x, c), dev(y, xn, c))

    def wait_stage1(h, t):
        d, k = t // CHUNKS, t % CHUNKS
        for slot in range(3):
            view = r1.at[h, slot, d, pl.ds(k * CH, CH)]
            pltpu.make_async_copy(view, view, s1_recv.at[h, slot, t]).wait()

    def start_loads(h, t, dest):
        d, k = t // CHUNKS, t % CHUNKS
        for j in range(CH):
            def start(src):
                pltpu.make_async_copy(src, ld.at[h, 3, j], ld_sem.at[h, 3]).start()
            by_block(cover_start(dest) + h * HALF + k * CH + j, sources, start)
        for slot in range(3):
            pltpu.make_async_copy(
                r1.at[h, slot, d, pl.ds(k * CH, CH)], ld.at[h, slot], ld_sem.at[h, slot]).start()

    def wait_loads(h):
        for slot in range(4):
            pltpu.make_async_copy(ld.at[h, slot], ld.at[h, slot], ld_sem.at[h, slot]).wait()

    def partial_sum(h, j, t0):
        rows = [ld[h, s, j, pl.ds(t0, 4)].astype(jnp.float32) for s in range(4)]
        return (rows[3] + rows[0]) + (rows[1] + rows[2])

    def stage2_copy(h, k):
        return pltpu.make_async_remote_copy(
            src_ref=st.at[h, k % SLOTS], dst_ref=r2.at[h, pl.ds(k * CH, CH)],
            send_sem=s2_send.at[h, k % SLOTS], recv_sem=s2_recv.at[h, k],
            device_id=(other[h],), device_id_type=MESH)

    def other_step(k, carry):
        issue(k + AHEAD)
        for h in HALVES:
            wait_stage1(h, k)
            start_loads(h, k, other[h])
        for h in HALVES:
            @pl.when(k >= SLOTS)
            def _():
                stage2_copy(h, k - SLOTS).wait_send()
            wait_loads(h)
            for j in range(CH):
                def add(i, z):
                    st[h, k % SLOTS, j, pl.ds(i * 4, 4)] = partial_sum(h, j, i * 4)
                    return z
                lax.fori_loop(0, 9, add, 0)
            stage2_copy(h, k).start()
        return carry

    lax.fori_loop(0, CHUNKS, other_step, 0)

    acc[...] = jnp.zeros_like(acc)
    first, last = own_start(me), own_start(me + 1)

    def g_copy(h, k):
        row = pl.multiple_of((h * HALF + k * CH) * ROWS, 8)
        return pltpu.make_async_copy(
            fbuf.at[h, k % 2], g_hbm.at[pl.ds(row, CH * ROWS)], g_sem.at[h, k % 2])

    def own_step(k, carry):
        t = k + CHUNKS
        issue(t + AHEAD)
        for h in HALVES:
            wait_stage1(h, t)
            view = r2.at[h, pl.ds(k * CH, CH)]
            pltpu.make_async_copy(view, view, s2_recv.at[h, k]).wait()
            start_loads(h, t, me)
            pltpu.make_async_copy(view, ld2.at[h], ld_sem.at[h, 4]).start()
        for h in HALVES:
            @pl.when(k >= 2)
            def _():
                g_copy(h, k - 2).wait()
            wait_loads(h)
            pltpu.make_async_copy(ld2.at[h], ld2.at[h], ld_sem.at[h, 4]).wait()
            for j in range(CH):
                b = cover_start(me) + h * HALF + k * CH + j
                weight = jnp.where((b >= first) & (b < last), 1.0, 0.0)

                def add(i, z):
                    s = partial_sum(h, j, i * 4) + ld2[h, j, pl.ds(i * 4, 4)]
                    sbuf[pl.ds(i * 4, 4)] = s
                    return z + jnp.sum(s * s, axis=0)
                sq = lax.fori_loop(0, 9, add, jnp.zeros((8, 128), jnp.float32))
                acc[...] += sq * weight
                dst = fbuf.at[h, k % 2, pl.ds(j * ROWS, ROWS)]
                is_row, is_gate, is_q, is_kv = kind_of(b)
                pl.when(is_row)(functools.partial(rows_to_joined, sbuf, dst))
                pl.when(is_gate)(functools.partial(transposed_to_joined, "gate", sbuf, tbuf, dst))
                pl.when(is_q)(functools.partial(transposed_to_joined, "q", sbuf, tbuf, dst))
                pl.when(is_kv)(functools.partial(transposed_to_joined, "kv", sbuf, tbuf, dst))
            g_copy(h, k).start()
        return carry

    lax.fori_loop(0, CHUNKS, own_step, 0)

    nbuf[me] = acc[...]

    def norm_copy(o):
        return pltpu.make_async_remote_copy(
            src_ref=acc, dst_ref=nbuf.at[me], send_sem=n_send.at[o - 1], recv_sem=n_recv.at[me],
            device_id=((me + o) % GROUP,), device_id_type=MESH)

    for o in OTHERS:
        norm_copy(o).start()
    for h in HALVES:
        for k in range(CHUNKS - 2, CHUNKS):
            g_copy(h, k).wait()
        for k in range(CHUNKS - SLOTS, CHUNKS):
            stage2_copy(h, k).wait_send()
        for n in STATE:
            for t in range(total_steps - SLOTS, total_steps):
                sent(h, n, t)
    for o in OTHERS:
        peer = (me + o) % GROUP
        pltpu.make_async_copy(nbuf.at[peer], nbuf.at[peer], n_recv.at[peer]).wait()
    for o in OTHERS:
        norm_copy(o).wait_send()
    total = nbuf[0]
    for i in OTHERS:
        total = total + nbuf[i]
    nrm_ref[...] = total


def run_reduce(sources):
    any_spec = pl.BlockSpec(memory_space=pl.ANY)
    f32, bf16 = jnp.float32, jnp.bfloat16
    tile = TILE
    out_shape = (
        jax.ShapeDtypeStruct((COVER * ROWS, 128), f32),
        jax.ShapeDtypeStruct((8, 128), f32),
        jax.ShapeDtypeStruct((2, 3, 2, HALF) + tile, bf16),
        jax.ShapeDtypeStruct((2, HALF) + tile, f32),
    )
    dma = pltpu.SemaphoreType.DMA
    outs = pl.pallas_call(
        reduce_kernel, out_shape=out_shape, in_specs=[any_spec] * len(sources),
        out_specs=(any_spec, pl.BlockSpec(memory_space=pltpu.VMEM), any_spec, any_spec),
        scratch_shapes=[
            pltpu.VMEM((2, 4, CH) + tile, bf16),
            pltpu.VMEM((2, CH) + tile, f32),
            pltpu.VMEM((2, SLOTS, CH) + tile, f32),
            pltpu.VMEM(tile, f32),
            pltpu.VMEM((3, 128, 128), f32),
            pltpu.VMEM((2, 2, CH * ROWS, 128), f32),
            pltpu.VMEM((8, 128), f32),
            pltpu.VMEM((GROUP, 8, 128), f32),
            dma((PAIR, 3, SLOTS)), dma((PAIR, 3, 2 * CHUNKS)), dma((PAIR, SLOTS)), dma((PAIR, CHUNKS)),
            dma((PAIR, 5)), dma((PAIR, 2)), dma((GROUP - 1,)), dma((GROUP,)),
        ],
        compiler_params=pltpu.CompilerParams(collective_id=0, has_side_effects=True),
        name="reduce_scatter",
    )(*sources)
    return outs[0], outs[1]


def update_kernel(hyper_ref, nrm_ref, g_hbm, m_hbm, v_hbm, p_hbm, mt, vt, pt,
                  m_out, v_out, p_out, o, gbuf, pbuf, fbuf, tbuf, cbuf, gin, sin, sout, obuf,
                  in_sem, out_sem, o_sem, f_send, f_recv, s_send, s_recv, p_send, p_recv):
    me = lax.axis_index("dp")
    y, x, c, xn, yn = positions(me)
    partner = dev(y, x, 1 - c)
    near = (dev(yn, x, c), dev(y, xn, c))
    far = dev(yn, xn, c)
    barrier = pltpu.get_barrier_semaphore()
    for device in (partner,) + near:
        pl.semaphore_signal(barrier, inc=1, device_id=(device,), device_id_type=MESH)
    pl.semaphore_wait(barrier, 3)

    lr, b1, b2, wd, max_norm = [hyper_ref[n] for n in range(5)]
    delta = me * SHARE - cover_start(me) * BLK
    rho, odd = delta // 128, me % 2 == 1
    sigma = (own_start(me) * BLK - me * SHARE) // 128
    low, high = pl.ds(0, ROWS), pl.ds(ROWS, ROWS)
    state, tails, outs = (m_hbm, v_hbm, p_hbm), (mt, vt, pt), (m_out, v_out, p_out)
    size = 32
    lane = lax.broadcasted_iota(jnp.int32, (size, 128), 1)
    sub = lax.broadcasted_iota(jnp.int32, (size, 128), 0)
    own_lane = (lane < 64) | jnp.logical_not(odd)

    def place(buf, at, count, value):
        @pl.when(odd)
        def _():
            buf[pl.ds(at, count), :] = pltpu.roll(value(), 64, 1)

        @pl.when(jnp.logical_not(odd))
        def _():
            buf[pl.ds(at, count), :] = value()

    def window(buf, row, j):
        at = row + size * j
        return jnp.where(own_lane, buf[pl.ds(at, size), :], buf[pl.ds(at + 1, size), :])

    def flat(i, n, first=0, count=BLK):
        return pl.ds(pl.multiple_of((i % 2 * 3 + n) * BLK + first, 1024), count)

    def span(i):
        return pl.ds(pl.multiple_of(i * BLK, 1024), BLK)

    def g_copy(i, slot):
        rows = pl.ds(pl.multiple_of(i * ROWS, 8), ROWS)
        return pltpu.make_async_copy(g_hbm.at[rows], gin.at[slot], in_sem.at[slot, 3])

    def start_loads(i):
        g_copy(i + 1, i % 2).start()
        for n in STATE:
            @pl.when(i < OWN - 1)
            def _():
                pltpu.make_async_copy(state[n].at[span(i)], sin.at[flat(i, n)], in_sem.at[i % 2, n]).start()

            @pl.when(i >= OWN - 1)
            def _():
                pltpu.make_async_copy(
                    tails[n].at[span(i - OWN + 1)], sin.at[flat(i, n)], in_sem.at[i % 2, n]).start()

    def store_copy(i, n):
        return pltpu.make_async_copy(sout.at[flat(i, n)], outs[n].at[span(i)], out_sem.at[i % 2, n])

    def block_copy(j):
        return pltpu.make_async_copy(
            obuf.at[j % SLOTS], o.at[me * OWN_HALF + j // 2, j % 2], o_sem.at[j % SLOTS])

    def step(i):
        @pl.when(i < OWN)
        def _():
            start_loads(i + 1)
        g_copy(i + 1, i % 2).wait()
        for n in STATE:
            view = sin.at[flat(i, n)]
            pltpu.make_async_copy(view, view, in_sem.at[i % 2, n]).wait()

            @pl.when((i >= 2) & (i < OWN))
            def _():
                store_copy(i - 2, n).wait()
        gbuf[low, :] = gbuf[high, :]
        pbuf[low, :] = pbuf[high, :]
        place(gbuf, ROWS, ROWS, lambda: gin[i % 2])
        scale, inv1, inv2 = [cbuf[n, :1] for n in STATE]
        keep = i < OWN
        for j in range(ROWS // size):
            first, count = size * 128 * j, size * 128
            h = window(gbuf, rho, j) * scale
            m, v, p = [sin[flat(i, n, first, count)].reshape(size, 128) for n in STATE]
            m1 = b1 * m + (1.0 - b1) * h
            v1 = b2 * v + (1.0 - b2) * (h * h)
            pos = me * SHARE + i * BLK + first + sub * 128 + lane
            decay = jnp.where(pos < DECAY_LEN, wd * p, 0.0)
            u = (m1 * inv1) / (jnp.sqrt(v1 * inv2) + ADAM_EPS) + decay
            p1 = p - lr * u
            place(pbuf, ROWS + size * j, size, lambda: p1)

            @pl.when(keep)
            def _():
                for n, value in enumerate((m1, v1, p1)):
                    sout[flat(i, n, first, count)] = value.reshape(count)

        @pl.when(keep)
        def _():
            for n in STATE:
                store_copy(i, n).start()

    def finish(i):
        j = i - 1
        for k in range(ROWS // size):
            fbuf[pl.ds(size * k, size), :] = window(pbuf, sigma, k)
        b = own_start(me) + j

        def emit(t, value):
            obuf[j % SLOTS, t] = value.astype(jnp.bfloat16)
        is_row, is_gate, is_q, is_kv = kind_of(b)
        pl.when(is_row)(functools.partial(joined_to_rows, fbuf, emit))
        pl.when(is_gate)(functools.partial(joined_to_transposed, "gate", fbuf, tbuf, emit))
        pl.when(is_q)(functools.partial(joined_to_transposed, "q", fbuf, tbuf, emit))
        pl.when(is_kv)(functools.partial(joined_to_transposed, "kv", fbuf, tbuf, emit))
        block_copy(j).start()

    def view(h, share, q, count):
        return o.at[pl.ds(share * OWN_HALF + q * CH, count), h]

    def copy(h, share, q, count, send, recv, device):
        span_ = view(h, share, q, count)
        pltpu.make_async_remote_copy(
            src_ref=span_, dst_ref=span_, send_sem=send, recv_sem=recv,
            device_id=(device,), device_id_type=MESH).start()

    def to_partner(h, which, q, count):
        share = (me, near[h], near[1 - h], far)[which]
        copy(h, share, q, count, p_send.at[h, which], p_recv.at[h, which, q], partner)

    def second_hop(h, which, q, count):
        share = (me, near[h])[which]
        copy(h, share, q, count, s_send.at[h, which], s_recv.at[h, which, q], near[1 - h])

    def arrived(h, count, sem):
        span_ = view(h, 0, 0, count)
        pltpu.make_async_copy(span_, span_, sem).wait()

    def send_own(q, count):
        for n in range(2 * count):
            block_copy(2 * CH * q + n).wait()
        for h in HALVES:
            copy(h, me, q, count, f_send.at[h], f_recv.at[h, q], near[h])
            second_hop(h, 0, q, count)
        for h in HALVES:
            to_partner(h, 0, q, count)

    def forward_near(q, count):
        for h in HALVES:
            arrived(h, count, f_recv.at[h, q])
            second_hop(h, 1, q, count)
            to_partner(h, 1, q, count)
        for h in HALVES:
            arrived(h, count, s_recv.at[h, 0, q])
            to_partner(h, 2, q, count)

    def forward_far(q, count):
        for h in HALVES:
            arrived(h, count, s_recv.at[h, 1, q])
            to_partner(h, 3, q, count)

    one = jnp.ones((8, 128), jnp.float32)

    def power(b):
        square = b * b
        cube = b * square
        return cube * (square * square)

    start_loads(jnp.int32(0))
    norm = jnp.sqrt(jnp.sum(nrm_ref[...], keepdims=True) * (1.0 / 64.0))
    clip = jnp.minimum(1.0, (one * max_norm) / (norm + CLIP_EPS))
    cbuf[0] = clip * 0.125
    cbuf[1] = one / (one * (1.0 - power(b1)))
    cbuf[2] = one / (one * (1.0 - power(b2)))
    g_copy(0, 2).start()
    g_copy(0, 2).wait()
    place(gbuf, ROWS, ROWS, lambda: gin[2])

    whole = OWN_HALF // CH
    step(jnp.int32(0))

    def inner(n, q):
        i = 2 * CH * q + n + 1
        step(i)
        finish(i)

        @pl.when((n == 0) & (q >= 1))
        def _():
            send_own(q - 1, CH)
        return q

    def outer(q, carry):
        lax.fori_loop(0, 2 * CH, inner, q)
        pl.when(q >= NEAR_LAG)(lambda: forward_near(q - NEAR_LAG, CH))
        pl.when(q >= FAR_LAG)(lambda: forward_far(q - FAR_LAG, CH))
        return carry

    lax.fori_loop(0, whole, outer, 0)
    send_own(whole - 1, CH)

    def last(i, carry):
        step(i)
        finish(i)
        return carry

    lax.fori_loop(OWN - 1, OWN + 1, last, 0)
    send_own(whole, 1)

    def rest(fn, first):
        def body(q, carry):
            fn(q, CH)
            return carry
        lax.fori_loop(first, whole, body, 0)
    rest(forward_near, whole - NEAR_LAG)
    forward_near(whole, 1)
    rest(forward_far, whole - FAR_LAG)
    forward_far(whole, 1)
    for i in (OWN - 2, OWN - 1):
        for n in STATE:
            store_copy(i, n).wait()

    def from_partner(q, count):
        for h in HALVES:
            for which in ALL:
                arrived(h, count, p_recv.at[h, which, q])
    rest(from_partner, 0)
    from_partner(whole, 1)
    for h in HALVES:
        arrived(h, OWN_HALF, f_send.at[h])
        for which in HALVES:
            arrived(h, OWN_HALF, s_send.at[h, which])
        for which in ALL:
            arrived(h, OWN_HALF, p_send.at[h, which])


def run_update(hyper, nrm, g, state, tails):
    f32, bf16, dma = jnp.float32, jnp.bfloat16, pltpu.SemaphoreType.DMA
    any_spec = pl.BlockSpec(memory_space=pl.ANY)
    chunks = OWN_HALF // CH + 1
    rows = pltpu.VMEM((2 * ROWS + 8, 128), f32)
    flat = pltpu.VMEM((6 * BLK,), f32)
    return pl.pallas_call(
        update_kernel,
        in_specs=[pl.BlockSpec(memory_space=pltpu.SMEM), pl.BlockSpec(memory_space=pltpu.VMEM)] + [any_spec] * 7,
        out_specs=[any_spec] * 4,
        out_shape=[jax.ShapeDtypeStruct((OWN * BLK,), f32)] * 3
        + [jax.ShapeDtypeStruct((GROUP * OWN_HALF, 2) + TILE, bf16)],
        scratch_shapes=[
            rows, rows, pltpu.VMEM((ROWS, 128), f32), pltpu.VMEM((3, 128, 128), f32),
            pltpu.VMEM((3, 8, 128), f32), pltpu.VMEM((3, ROWS, 128), f32), flat, flat,
            pltpu.VMEM((SLOTS,) + TILE, bf16),
            dma((3, 4)), dma((PAIR, 3)), dma((SLOTS,)), dma((PAIR,)), dma((PAIR, chunks)), dma((PAIR, 2)),
            dma((PAIR, 2, chunks)), dma((PAIR, 4)), dma((PAIR, 4, chunks))],
        compiler_params=pltpu.CompilerParams(collective_id=1, has_side_effects=True),
        name="update_gather",
    )(hyper, nrm, g, *state, *tails)


def pack(grads):
    embed, q, k, v, out, gate, up, down, norms, qk = [g[0] for g in grads]

    def rows(a):
        return a.reshape(-1, 8, COLS, 128).transpose(0, 2, 1, 3)

    def grid(a):
        layers, wide, high = a.shape
        return a.transpose(0, 2, 1).reshape(layers, high // 8, 8, COLS, 128).transpose(0, 1, 3, 2, 4)

    def cols(a, parts):
        a = grid(a)
        a = a.reshape(a.shape[0], a.shape[1], parts, -1, 8, 128).swapaxes(1, 2)
        return a.reshape((-1,) + TILE)

    tail = jnp.concatenate([norms.reshape(-1), qk.reshape(-1)])
    tail = jnp.pad(tail, (0, TAIL_BLOCKS * BLK - tail.shape[0]))
    small = jnp.concatenate([cols(q, 4), cols(k, 2), cols(v, 2), rows(out)])
    return rows(embed), small, grid(gate), grid(up), rows(down), rows(tail.reshape(-1, 4608))


def block_runs(b0, b1):
    cuts = [own_start(r) for r in range(GROUP + 1)]
    out = []
    for r in range(GROUP):
        lo, hi = max(b0, cuts[r]), min(b1, cuts[r + 1])
        if lo < hi:
            out.append((r * OWN + lo - cuts[r], hi - lo))
    return out


def unpack_kernel(o, embed, q, k, v, out, gate, up, down, tail, buf, in_sem, out_sem):
    def rows_out(ref, first):
        def store(slot, count):
            pltpu.make_async_copy(
                buf.at[slot, pl.ds(0, count)], ref.at[pl.ds(first, count)], out_sem.at[slot]).start()
        return store

    def grid_out(ref, layer):
        def store(slot, count):
            def one(rt, z):
                pltpu.make_async_copy(buf.at[slot, :, rt], ref.at[layer, rt], out_sem.at[slot]).start()
                return z
            lax.fori_loop(0, COLS, one, 0)
        return store

    def cols_out(ref, parts):
        high, wide = ref.shape[1], COLS // parts

        def store(slot, count):
            def one(n, z):
                for rt in range(high):
                    pltpu.make_async_copy(
                        buf.at[slot, n, pl.ds(wide * rt, wide)],
                        ref.at[n // parts, rt, pl.ds((n % parts) * wide, wide)], out_sem.at[slot]).start()
                return z
            lax.fori_loop(0, count, one, 0)
        return store

    jobs = []

    def add_rows(ref, b0, b1):
        for lo in range(b0, b1, COLS):
            hi = min(lo + COLS, b1)
            jobs.append((lo, hi - lo, rows_out(ref, lo - b0)))

    e = EDGES
    add_rows(embed, e[0], e[1])
    for layer in range(gate.shape[0]):
        jobs.append((e[5] + COLS * layer, COLS, grid_out(gate, layer)))
        jobs.append((e[6] + COLS * layer, COLS, grid_out(up, layer)))
    jobs.append((e[1], e[2] - e[1], cols_out(q, 4)))
    jobs.append((e[2], e[3] - e[2], cols_out(k, 2)))
    jobs.append((e[3], e[4] - e[3], cols_out(v, 2)))
    add_rows(out, e[4], e[5])
    add_rows(down, e[7], e[8])
    add_rows(tail, e[8], e[9])
    depth = buf.shape[0]

    def load(n):
        b0, count, _ = jobs[n]
        at = 0
        for first, size in block_runs(b0, b0 + count):
            pltpu.make_async_copy(
                o.at[pl.ds(first, size)], buf.at[n % depth, pl.ds(at, size)], in_sem.at[n % depth]).start()
            at += size

    def wait(n, sem):
        view = buf.at[n % depth, pl.ds(0, jobs[n][1])]
        pltpu.make_async_copy(view, view, sem.at[n % depth]).wait()

    lead = depth // 2
    for n in range(len(jobs) + lead):
        if n < len(jobs):
            if n >= depth:
                wait(n - depth, out_sem)
            load(n)
        if n >= lead:
            wait(n - lead, in_sem)
            jobs[n - lead][2]((n - lead) % depth, jobs[n - lead][1])
    for n in range(len(jobs) - depth, len(jobs)):
        wait(n, out_sem)


def run_unpack(o, shapes):
    e, bf16 = EDGES, jnp.bfloat16
    any_spec = pl.BlockSpec(memory_space=pl.ANY)

    def rows(n):
        return (n,) + TILE

    def grid(shape):
        return (shape[0], shape[2] // 8) + TILE
    views = [rows(e[1]), grid(shapes[1]), grid(shapes[2]), grid(shapes[3]), rows(e[5] - e[4]),
             grid(shapes[5]), grid(shapes[6]), rows(e[8] - e[7]), rows(e[9] - e[8])]
    dma = pltpu.SemaphoreType.DMA
    depth = 6
    outs = pl.pallas_call(
        unpack_kernel, out_shape=[jax.ShapeDtypeStruct(s, bf16) for s in views],
        in_specs=[any_spec], out_specs=[any_spec] * len(views),
        scratch_shapes=[pltpu.VMEM((depth, COLS) + TILE, bf16), dma((depth,)), dma((depth,))],
        name="unpack",
    )(o)

    def from_rows(a, shape):
        return a.swapaxes(1, 2).reshape(shape)

    def from_grid(a, shape):
        layers, wide, high = shape
        return a.swapaxes(2, 3).reshape(layers, high, wide).swapaxes(1, 2)
    params = [(from_grid if len(a.shape) > 4 else from_rows)(a, s) for a, s in zip(outs[:8], shapes)]
    tail = from_rows(outs[8], (-1,))
    size = math.prod(shapes[8])
    params.append(tail[:size].reshape(shapes[8]))
    params.append(tail[size:size + math.prod(shapes[9])].reshape(shapes[9]))
    return tuple(params)


def solution(mesh):
    group_size = mesh.shape["dp"]
    assert group_size == GROUP

    def local_update(*arrays):
        grads = arrays[:GRAD_COUNT]
        first_part, second_part, master_part, hyper_params = arrays[GRAD_COUNT:]
        state = (first_part, second_part, master_part)
        shapes = [grad_arr.shape[1:] for grad_arr in grads]

        heads = jnp.concatenate([s[:BLK] for s in state])
        heads = lax.ppermute(heads, "dp", [(r + 1, r) for r in range(GROUP - 1)])
        rest = 2 * BLK - (SHARE - 121 * BLK) - BLK
        tails = [jnp.concatenate([s[121 * BLK:], heads[n * BLK:(n + 1) * BLK], jnp.zeros((rest,), s.dtype)])
                 for n, s in enumerate(state)]

        g, nrm = run_reduce(pack(grads))
        *moved, o = run_update(hyper_params, nrm, g, state, tails)
        params = run_unpack(o.reshape((-1,) + TILE), shapes)
        return params + tuple(a[:SHARE] for a in moved)

    in_specs = tuple([P("dp")] * GRAD_COUNT + [P("dp"), P("dp"), P("dp"), P()])
    out_specs = tuple([P()] * GRAD_COUNT + [P("dp"), P("dp"), P("dp")])
    return jax.shard_map(local_update, mesh=mesh, in_specs=in_specs, out_specs=out_specs, check_vma=False)
```

```python
import functools
import math
import jax
import jax.numpy as jnp
from jax import lax
from jax.experimental import pallas as pl
from jax.experimental.pallas import tpu as pltpu
from jax.sharding import PartitionSpec as P

ADAM_STEP = 7
ADAM_EPS = 1e-8
CLIP_EPS = 1e-6
GRAD_COUNT = 10
NORM_COUNT = 2
MESH = pl.DeviceIdType.MESH

GROUP = 8
PAIR = 2
HALVES = range(PAIR)
OTHERS = range(1, GROUP)
STATE = range(3)
ALL = range(4)
BLK = 36864
ROWS = 288
SHARE = 4483776
HALF = 62
COVER = 2 * HALF
CH = 2
CHUNKS = HALF // CH
AHEAD = 3
SLOTS = 8
OWN = 122
OWN_HALF = OWN // 2
EDGES = (0, 250, 274, 286, 298, 322, 538, 754, 970, 976)
TAIL_BLOCKS = 6
TILE = (36, 8, 128)
COLS = 36
NEAR_LAG = 2
FAR_LAG = 4
PART = 2
DECAY_LEN = 970 * BLK


def cover_start(r):
    return (r * SHARE) // BLK


def own_start(r):
    return (r * SHARE + BLK - 1) // BLK


def kind_of(b):
    is_q = (b >= EDGES[1]) & (b < EDGES[2])
    is_kv = (b >= EDGES[2]) & (b < EDGES[4])
    is_gate = (b >= EDGES[5]) & (b < EDGES[7])
    is_row = (b < EDGES[1]) | ((b >= EDGES[4]) & (b < EDGES[5])) | (b >= EDGES[7])
    return is_row, is_gate, is_q, is_kv


def lane_pick(parts, width):
    lane = lax.broadcasted_iota(jnp.int32, parts[0].shape, 1)
    out = parts[0]
    for i in range(1, len(parts)):
        out = jnp.where(lane >= i * width, parts[i], out)
    return out


def roll_to(x, src, dst):
    shift = (dst - src) % 128
    return pltpu.roll(x, shift, 1) if shift else x


def tile_order(kind):
    if kind == "gate":
        return list(range(36))
    if kind == "q":
        return [rt * 9 + ct for ct in range(9) for rt in range(4)]
    return [rt * 18 + ct for ct in range(18) for rt in HALVES]


def pieces(kind):
    out = []
    if kind == "gate":
        for f in range(9):
            for q in range(4):
                k = 4 * f + q
                dd, a = k // 9, k % 9
                out.append(((f, 32, 9), q, (a // 4, dd, 4), a % 4))
    elif kind == "q":
        for ct in range(9):
            for q in range(4):
                out.append(((32 * ct, 32, 1), q, (ct // 4, q, 4), ct % 4))
    else:
        for ct in range(18):
            for q in range(8):
                out.append(((16 * ct, 16, 1), q, (ct // 8, q, 8), ct % 8))
    return out


def width_of(kind):
    return 16 if kind == "kv" else 32


def rows_to_joined(src, dst):
    for i in range(8):
        dst[pl.ds(36 * i, 36), :] = src[:, i, :]


def joined_to_rows(src, emit):
    for t in range(36):
        emit(t, src[pl.ds(t, 8, stride=36), :])


def transposed_to_joined(kind, src, tbuf, dst):
    order = tile_order(kind)
    for j in range(3):
        tiles = [src[t] for t in order[16 * j:16 * j + 16]]
        if len(tiles) < 16:
            tiles.append(jnp.zeros((128 - 8 * len(tiles), 128), jnp.float32))
        tbuf[j] = jnp.concatenate(tiles, axis=0).T
    w = width_of(kind)
    groups = {}
    for drows, dl, srows, sl in pieces(kind):
        groups.setdefault(drows, []).append((dl, srows, sl))
    for (start, count, stride), items in groups.items():
        parts = [None] * (128 // w)
        for dl, (g, s0, sstr), sl in items:
            parts[dl] = roll_to(tbuf[g, pl.ds(s0, count, stride=sstr), :], sl * w, dl * w)
        value = lane_pick(parts, w)
        if stride == 1:
            dst[pl.ds(start, count), :] = value
        else:
            dst[pl.ds(start, count, stride=stride), :] = value


def joined_to_transposed(kind, src, tbuf, emit):
    order = tile_order(kind)
    w = width_of(kind)
    groups = {}
    for drows, dl, srows, sl in pieces(kind):
        groups.setdefault(srows, []).append((sl, drows, dl))
    for (g, s0, sstr), items in groups.items():
        count = items[0][1][1]
        parts = [None] * (128 // w)
        for sl, (start, cnt, stride), dl in items:
            if stride == 1:
                rows = src[pl.ds(start, cnt), :]
            else:
                rows = src[pl.ds(start, cnt, stride=stride), :]
            parts[sl] = roll_to(rows, dl * w, sl * w)
        filler = next(p for p in parts if p is not None)
        parts = [filler if p is None else p for p in parts]
        tbuf[g, pl.ds(s0, count, stride=sstr), :] = lane_pick(parts, w)
    for j in range(3):
        block = tbuf[j].T
        for n, t in enumerate(order[16 * j:16 * j + 16]):
            emit(t, block[8 * n:8 * n + 8, :])


def positions(me):
    y, x, c = me // 4, (me // 2) % 2, me % 2
    xn, yn = 1 - x, 1 - y
    return y, x, c, xn, yn


def dev(y, x, c):
    return (y * 2 + x) * 2 + c


def by_block(b, refs, fn):
    for kind, ref in enumerate(refs):
        first, last = EDGES[kind], EDGES[kind + 1]
        shape = ref.shape

        @pl.when((b >= first) & (b < last))
        def _(ref=ref, shape=shape, n=b - first):
            if len(shape) == 4:
                fn(ref.at[n], 0, COLS)
                return
            high = shape[1]
            wide = COLS // high
            layer, part = n // high, n % high
            if wide == 1:
                fn(ref.at[layer, :, part], 0, COLS)
            else:
                for rt in range(high):
                    fn(ref.at[layer, rt, pl.ds(part * wide, wide)], rt * wide, wide)


def reduce_kernel(e_in, q_in, k_in, v_in, o_in, gate_in, up_in, down_in, tail_in, g_hbm, nrm_ref, r1, r2, ld, ld2, st, sbuf, tbuf, fbuf, acc, nbuf,
                  s1_send, s1_recv, s2_send, s2_recv, ld_sem, g_sem, n_send, n_recv):
    me = lax.axis_index("dp")
    y, x, c, xn, yn = positions(me)
    sources = (e_in, q_in, k_in, v_in, o_in, gate_in, up_in, down_in, tail_in)
    barrier = pltpu.get_barrier_semaphore()
    for o in OTHERS:
        pl.semaphore_signal(barrier, inc=1, device_id=((me + o) % GROUP,), device_id_type=MESH)
    pl.semaphore_wait(barrier, GROUP - 1)

    partner = dev(y, x, 1 - c)
    def targets(h):
        cy, cx = (y, xn) if h == 0 else (yn, x)
        oy, ox = (1 - cy, cx) if h == 0 else (cy, 1 - cx)
        py, px = (1 - y, x) if h == 0 else (y, 1 - x)
        return (
            (partner, 0, (dev(py, px, 1 - c), partner)),
            (dev(cy, cx, 0), 1 + c, (dev(oy, ox, 0), dev(cy, cx, 0))),
            (dev(cy, cx, 1), 1 + c, (dev(oy, ox, 1), dev(cy, cx, 1))),
        )

    def send(h, n, t):
        d, k = t // CHUNKS, t % CHUNKS
        device, slot, dests = targets(h)[n]
        dest = dests[0] * (1 - d) + dests[1] * d
        for j in range(CH):
            at = k * CH + j

            def start(src, tile, tiles):
                pltpu.make_async_remote_copy(
                    src_ref=src, dst_ref=r1.at[h, slot, d, at, pl.ds(tile, tiles)],
                    send_sem=s1_send.at[h, n, t % SLOTS], recv_sem=s1_recv.at[h, slot, t],
                    device_id=(device,), device_id_type=MESH).start()
            by_block(cover_start(dest) + h * HALF + at, sources, start)

    def sent(h, n, t):
        view = ld.at[h, 0]
        pltpu.make_async_copy(view, view, s1_send.at[h, n, t % SLOTS]).wait()

    total_steps = 2 * CHUNKS

    def issue(t):
        @pl.when(t < total_steps)
        def _():
            for n in (1, 2, 0):
                for h in HALVES:
                    @pl.when(t >= SLOTS)
                    def _():
                        sent(h, n, t - SLOTS)
                    send(h, n, t)

    def first_issue(t, carry):
        issue(t)
        return carry

    lax.fori_loop(0, AHEAD, first_issue, 0)

    other = (dev(yn, x, c), dev(y, xn, c))

    def wait_stage1(h, t):
        d, k = t // CHUNKS, t % CHUNKS
        for slot in range(3):
            view = r1.at[h, slot, d, pl.ds(k * CH, CH)]
            pltpu.make_async_copy(view, view, s1_recv.at[h, slot, t]).wait()

    def start_loads(h, t, dest):
        d, k = t // CHUNKS, t % CHUNKS
        for j in range(CH):
            def start(src, tile, tiles):
                pltpu.make_async_copy(
                    src, ld.at[h, 3, j, pl.ds(tile, tiles)], ld_sem.at[h, 3]).start()
            by_block(cover_start(dest) + h * HALF + k * CH + j, sources, start)
        for slot in range(3):
            pltpu.make_async_copy(
                r1.at[h, slot, d, pl.ds(k * CH, CH)], ld.at[h, slot], ld_sem.at[h, slot]).start()

    def wait_loads(h):
        for slot in range(4):
            pltpu.make_async_copy(ld.at[h, slot], ld.at[h, slot], ld_sem.at[h, slot]).wait()

    def partial_sum(h, j, t0):
        rows = [ld[h, s, j, pl.ds(t0, 4)].astype(jnp.float32) for s in range(4)]
        return (rows[3] + rows[0]) + (rows[1] + rows[2])

    def stage2_copy(h, k):
        return pltpu.make_async_remote_copy(
            src_ref=st.at[h, k % SLOTS], dst_ref=r2.at[h, pl.ds(k * CH, CH)],
            send_sem=s2_send.at[h, k % SLOTS], recv_sem=s2_recv.at[h, k],
            device_id=(other[h],), device_id_type=MESH)

    def other_step(k, carry):
        issue(k + AHEAD)
        for h in HALVES:
            wait_stage1(h, k)
            start_loads(h, k, other[h])
        for h in HALVES:
            @pl.when(k >= SLOTS)
            def _():
                stage2_copy(h, k - SLOTS).wait_send()
            wait_loads(h)
            for j in range(CH):
                def add(i, z):
                    st[h, k % SLOTS, j, pl.ds(i * 4, 4)] = partial_sum(h, j, i * 4)
                    return z
                lax.fori_loop(0, 9, add, 0)
            stage2_copy(h, k).start()
        return carry

    lax.fori_loop(0, CHUNKS, other_step, 0)

    acc[...] = jnp.zeros_like(acc)
    first, last = own_start(me), own_start(me + 1)

    def g_copy(h, k):
        row = pl.multiple_of((h * HALF + k * CH) * ROWS, 8)
        return pltpu.make_async_copy(
            fbuf.at[h, k % 2], g_hbm.at[pl.ds(row, CH * ROWS)], g_sem.at[h, k % 2])

    def own_step(k, carry):
        t = k + CHUNKS
        issue(t + AHEAD)
        for h in HALVES:
            wait_stage1(h, t)
            view = r2.at[h, pl.ds(k * CH, CH)]
            pltpu.make_async_copy(view, view, s2_recv.at[h, k]).wait()
            start_loads(h, t, me)
            pltpu.make_async_copy(view, ld2.at[h], ld_sem.at[h, 4]).start()
        for h in HALVES:
            @pl.when(k >= 2)
            def _():
                g_copy(h, k - 2).wait()
            wait_loads(h)
            pltpu.make_async_copy(ld2.at[h], ld2.at[h], ld_sem.at[h, 4]).wait()
            for j in range(CH):
                b = cover_start(me) + h * HALF + k * CH + j
                weight = jnp.where((b >= first) & (b < last), 1.0, 0.0)

                def add(i, z):
                    s = partial_sum(h, j, i * 4) + ld2[h, j, pl.ds(i * 4, 4)]
                    sbuf[pl.ds(i * 4, 4)] = s
                    return z + jnp.sum(s * s, axis=0)
                sq = lax.fori_loop(0, 9, add, jnp.zeros((8, 128), jnp.float32))
                acc[...] += sq * weight
                dst = fbuf.at[h, k % 2, pl.ds(j * ROWS, ROWS)]
                is_row, is_gate, is_q, is_kv = kind_of(b)
                pl.when(is_row)(functools.partial(rows_to_joined, sbuf, dst))
                pl.when(is_gate)(functools.partial(transposed_to_joined, "gate", sbuf, tbuf, dst))
                pl.when(is_q)(functools.partial(transposed_to_joined, "q", sbuf, tbuf, dst))
                pl.when(is_kv)(functools.partial(transposed_to_joined, "kv", sbuf, tbuf, dst))
            g_copy(h, k).start()
        return carry

    lax.fori_loop(0, CHUNKS, own_step, 0)

    nbuf[me] = acc[...]

    def norm_copy(o):
        return pltpu.make_async_remote_copy(
            src_ref=acc, dst_ref=nbuf.at[me], send_sem=n_send.at[o - 1], recv_sem=n_recv.at[me],
            device_id=((me + o) % GROUP,), device_id_type=MESH)

    for o in OTHERS:
        norm_copy(o).start()
    for h in HALVES:
        for k in range(CHUNKS - 2, CHUNKS):
            g_copy(h, k).wait()
        for k in range(CHUNKS - SLOTS, CHUNKS):
            stage2_copy(h, k).wait_send()
        for n in STATE:
            for t in range(total_steps - SLOTS, total_steps):
                sent(h, n, t)
    for o in OTHERS:
        peer = (me + o) % GROUP
        pltpu.make_async_copy(nbuf.at[peer], nbuf.at[peer], n_recv.at[peer]).wait()
    for o in OTHERS:
        norm_copy(o).wait_send()
    total = nbuf[0]
    for i in OTHERS:
        total = total + nbuf[i]
    nrm_ref[...] = total


def run_reduce(sources):
    any_spec = pl.BlockSpec(memory_space=pl.ANY)
    f32, bf16 = jnp.float32, jnp.bfloat16
    tile = TILE
    out_shape = (
        jax.ShapeDtypeStruct((COVER * ROWS, 128), f32),
        jax.ShapeDtypeStruct((8, 128), f32),
        jax.ShapeDtypeStruct((2, 3, 2, HALF) + tile, bf16),
        jax.ShapeDtypeStruct((2, HALF) + tile, f32),
    )
    dma = pltpu.SemaphoreType.DMA
    outs = pl.pallas_call(
        reduce_kernel, out_shape=out_shape, in_specs=[any_spec] * len(sources),
        out_specs=(any_spec, pl.BlockSpec(memory_space=pltpu.VMEM), any_spec, any_spec),
        scratch_shapes=[
            pltpu.VMEM((2, 4, CH) + tile, bf16),
            pltpu.VMEM((2, CH) + tile, f32),
            pltpu.VMEM((2, SLOTS, CH) + tile, f32),
            pltpu.VMEM(tile, f32),
            pltpu.VMEM((3, 128, 128), f32),
            pltpu.VMEM((2, 2, CH * ROWS, 128), f32),
            pltpu.VMEM((8, 128), f32),
            pltpu.VMEM((GROUP, 8, 128), f32),
            dma((PAIR, 3, SLOTS)), dma((PAIR, 3, 2 * CHUNKS)), dma((PAIR, SLOTS)), dma((PAIR, CHUNKS)),
            dma((PAIR, 5)), dma((PAIR, 2)), dma((GROUP - 1,)), dma((GROUP,)),
        ],
        compiler_params=pltpu.CompilerParams(collective_id=0, has_side_effects=True),
        name="reduce_scatter",
    )(*sources)
    return outs[0], outs[1]


def update_kernel(hyper_ref, nrm_ref, g_hbm, m_hbm, v_hbm, p_hbm, mt, vt, pt,
                  m_out, v_out, p_out, o, gbuf, pbuf, fbuf, tbuf, cbuf, gin, sin, sout, obuf,
                  in_sem, out_sem, o_sem, f_send, f_recv, s_send, s_recv, p_send, p_recv):
    me = lax.axis_index("dp")
    y, x, c, xn, yn = positions(me)
    partner = dev(y, x, 1 - c)
    near = (dev(yn, x, c), dev(y, xn, c))
    far = dev(yn, xn, c)
    barrier = pltpu.get_barrier_semaphore()
    for device in (partner,) + near:
        pl.semaphore_signal(barrier, inc=1, device_id=(device,), device_id_type=MESH)
    pl.semaphore_wait(barrier, 3)

    lr, b1, b2, wd, max_norm = [hyper_ref[n] for n in range(5)]
    delta = me * SHARE - cover_start(me) * BLK
    rho, odd = delta // 128, me % 2 == 1
    sigma = (own_start(me) * BLK - me * SHARE) // 128
    low, high = pl.ds(0, ROWS), pl.ds(ROWS, ROWS)
    state, tails, outs = (m_hbm, v_hbm, p_hbm), (mt, vt, pt), (m_out, v_out)
    size = 32
    lane = lax.broadcasted_iota(jnp.int32, (size, 128), 1)
    sub = lax.broadcasted_iota(jnp.int32, (size, 128), 0)
    own_lane = (lane < 64) | jnp.logical_not(odd)

    def place(buf, at, count, value):
        @pl.when(odd)
        def _():
            buf[pl.ds(at, count), :] = pltpu.roll(value(), 64, 1)

        @pl.when(jnp.logical_not(odd))
        def _():
            buf[pl.ds(at, count), :] = value()

    def window(buf, row, j):
        at = row + size * j
        return jnp.where(own_lane, buf[pl.ds(at, size), :], buf[pl.ds(at + 1, size), :])

    def flat(i, n, first=0, count=BLK):
        return pl.ds(pl.multiple_of((i % 2 * 3 + n) * BLK + first, 1024), count)

    def span(i):
        return pl.ds(pl.multiple_of(i * BLK, 1024), BLK)

    def g_copy(i, slot):
        rows = pl.ds(pl.multiple_of(i * ROWS, 8), ROWS)
        return pltpu.make_async_copy(g_hbm.at[rows], gin.at[slot], in_sem.at[slot, 3])

    def start_loads(i):
        g_copy(i + 1, i % 2).start()
        for n in STATE:
            @pl.when(i < OWN - 1)
            def _():
                pltpu.make_async_copy(state[n].at[span(i)], sin.at[flat(i, n)], in_sem.at[i % 2, n]).start()

            @pl.when(i >= OWN - 1)
            def _():
                pltpu.make_async_copy(
                    tails[n].at[span(i - OWN + 1)], sin.at[flat(i, n)], in_sem.at[i % 2, n]).start()

    def store_copy(i):
        return pltpu.make_async_copy(
            sout.at[pl.ds(pl.multiple_of(i % 2 * BLK, 1024), BLK)], p_out.at[span(i)], out_sem.at[i % 2])

    def block_copy(j):
        return pltpu.make_async_copy(
            obuf.at[j % SLOTS], o.at[me * OWN_HALF + j // 2, j % 2], o_sem.at[j % SLOTS])

    def step(i):
        @pl.when(i < OWN)
        def _():
            start_loads(i + 1)
        g_copy(i + 1, i % 2).wait()
        for n in STATE:
            view = sin.at[flat(i, n)]
            pltpu.make_async_copy(view, view, in_sem.at[i % 2, n]).wait()
        pl.when(i >= 2)(lambda: store_copy(i - 2).wait())
        gbuf[low, :] = gbuf[high, :]
        pbuf[low, :] = pbuf[high, :]
        place(gbuf, ROWS, ROWS, lambda: gin[i % 2])
        scale, inv1, inv2 = [cbuf[n, :1] for n in STATE]
        for j in range(ROWS // size):
            first, count = size * 128 * j, size * 128
            h = window(gbuf, rho, j) * scale
            m, v, p = [sin[flat(i, n, first, count)].reshape(size, 128) for n in STATE]
            m1 = b1 * m + (1.0 - b1) * h
            v1 = b2 * v + (1.0 - b2) * (h * h)
            pos = me * SHARE + i * BLK + first + sub * 128 + lane
            decay = jnp.where(pos < DECAY_LEN, wd * p, 0.0)
            u = (m1 * inv1) / (jnp.sqrt(v1 * inv2) + ADAM_EPS) + decay
            p1 = p - lr * u
            place(pbuf, ROWS + size * j, size, lambda: p1)
            sout[pl.ds(pl.multiple_of(i % 2 * BLK + first, 1024), count)] = p1.reshape(count)

            @pl.when(i < OWN)
            def _():
                for n, value in enumerate((m1, v1)):
                    outs[n][pl.ds(pl.multiple_of(i * BLK + first, 1024), count)] = value.reshape(count)

        pl.when(i < OWN)(lambda: store_copy(i).start())

    def finish(i):
        j = i - 1
        for k in range(ROWS // size):
            fbuf[pl.ds(size * k, size), :] = window(pbuf, sigma, k)
        b = own_start(me) + j

        def emit(t, value):
            obuf[j % SLOTS, t] = value.astype(jnp.bfloat16)
        is_row, is_gate, is_q, is_kv = kind_of(b)
        pl.when(is_row)(functools.partial(joined_to_rows, fbuf, emit))
        pl.when(is_gate)(functools.partial(joined_to_transposed, "gate", fbuf, tbuf, emit))
        pl.when(is_q)(functools.partial(joined_to_transposed, "q", fbuf, tbuf, emit))
        pl.when(is_kv)(functools.partial(joined_to_transposed, "kv", fbuf, tbuf, emit))
        block_copy(j).start()

    def view(h, share, q, count):
        return o.at[pl.ds(share * OWN_HALF + q * PART, count), h]

    def copy(h, share, q, count, send, recv, device):
        span_ = view(h, share, q, count)
        pltpu.make_async_remote_copy(
            src_ref=span_, dst_ref=span_, send_sem=send, recv_sem=recv,
            device_id=(device,), device_id_type=MESH).start()

    def to_partner(h, which, q, count):
        share = (me, near[h], near[1 - h], far)[which]
        copy(h, share, q, count, p_send.at[h, which], p_recv.at[h, which, q], partner)

    def second_hop(h, which, q, count):
        share = (me, near[h])[which]
        copy(h, share, q, count, s_send.at[h, which], s_recv.at[h, which, q], near[1 - h])

    def arrived(h, count, sem):
        span_ = view(h, 0, 0, count)
        pltpu.make_async_copy(span_, span_, sem).wait()

    def send_own(q, count):
        for n in range(2 * count):
            block_copy(2 * PART * q + n).wait()
        for h in HALVES:
            copy(h, me, q, count, f_send.at[h], f_recv.at[h, q], near[h])
            second_hop(h, 0, q, count)
        for h in HALVES:
            to_partner(h, 0, q, count)

    def forward_near(q, count):
        for h in HALVES:
            arrived(h, count, f_recv.at[h, q])
            second_hop(h, 1, q, count)
            to_partner(h, 1, q, count)
        for h in HALVES:
            arrived(h, count, s_recv.at[h, 0, q])
            to_partner(h, 2, q, count)

    def forward_far(q, count):
        for h in HALVES:
            arrived(h, count, s_recv.at[h, 1, q])
            to_partner(h, 3, q, count)

    one = jnp.ones((8, 128), jnp.float32)

    def power(b):
        square = b * b
        cube = b * square
        return cube * (square * square)

    start_loads(jnp.int32(0))
    norm = jnp.sqrt(jnp.sum(nrm_ref[...], keepdims=True) * (1.0 / 64.0))
    clip = jnp.minimum(1.0, (one * max_norm) / (norm + CLIP_EPS))
    cbuf[0] = clip * 0.125
    cbuf[1] = one / (one * (1.0 - power(b1)))
    cbuf[2] = one / (one * (1.0 - power(b2)))
    g_copy(0, 2).start()
    g_copy(0, 2).wait()
    place(gbuf, ROWS, ROWS, lambda: gin[2])

    whole = (OWN_HALF - 1) // PART
    step(jnp.int32(0))

    def inner(n, q):
        i = 2 * PART * q + n + 1
        step(i)
        finish(i)

        @pl.when((n == 0) & (q >= 1))
        def _():
            send_own(q - 1, PART)
        return q

    def outer(q, carry):
        lax.fori_loop(0, 2 * PART, inner, q)
        pl.when(q >= NEAR_LAG)(lambda: forward_near(q - NEAR_LAG, PART))
        pl.when(q >= FAR_LAG)(lambda: forward_far(q - FAR_LAG, PART))
        return carry

    lax.fori_loop(0, whole, outer, 0)
    send_own(whole - 1, PART)

    def last(i, carry):
        step(i)
        finish(i)
        return carry

    lax.fori_loop(OWN - 1, OWN + 1, last, 0)
    send_own(whole, 1)

    def rest(fn, first):
        def body(q, carry):
            fn(q, PART)
            return carry
        lax.fori_loop(first, whole, body, 0)
    rest(forward_near, whole - NEAR_LAG)
    forward_near(whole, 1)
    rest(forward_far, whole - FAR_LAG)
    forward_far(whole, 1)

    store_copy(OWN - 1).wait()

    def from_partner(q, count):
        for h in HALVES:
            for which in ALL:
                arrived(h, count, p_recv.at[h, which, q])
    rest(from_partner, 0)
    from_partner(whole, 1)
    for h in HALVES:
        arrived(h, OWN_HALF, f_send.at[h])
        for which in HALVES:
            arrived(h, OWN_HALF, s_send.at[h, which])
        for which in ALL:
            arrived(h, OWN_HALF, p_send.at[h, which])


def run_update(hyper, nrm, g, state, tails):
    f32, bf16, dma = jnp.float32, jnp.bfloat16, pltpu.SemaphoreType.DMA
    any_spec = pl.BlockSpec(memory_space=pl.ANY)
    chunks = (OWN_HALF - 1) // PART + 1
    rows = pltpu.VMEM((2 * ROWS + 8, 128), f32)
    flat = pltpu.VMEM((6 * BLK,), f32)
    return pl.pallas_call(
        update_kernel,
        in_specs=[pl.BlockSpec(memory_space=pltpu.SMEM), pl.BlockSpec(memory_space=pltpu.VMEM)] + [any_spec] * 7,
        out_specs=[pl.BlockSpec(memory_space=pltpu.VMEM)] * PAIR + [any_spec] * PAIR,
        out_shape=[pltpu.VMEM((OWN * BLK,), f32)] * PAIR + [jax.ShapeDtypeStruct((OWN * BLK,), f32)]
        + [jax.ShapeDtypeStruct((GROUP * OWN_HALF, 2) + TILE, bf16)],
        scratch_shapes=[
            rows, rows, pltpu.VMEM((ROWS, 128), f32), pltpu.VMEM((3, 128, 128), f32),
            pltpu.VMEM((3, 8, 128), f32), pltpu.VMEM((3, ROWS, 128), f32), flat, pltpu.VMEM((PAIR * BLK,), f32),
            pltpu.VMEM((SLOTS,) + TILE, bf16),
            dma((3, 4)), dma((PAIR,)), dma((SLOTS,)), dma((PAIR,)), dma((PAIR, chunks)), dma((PAIR, 2)),
            dma((PAIR, 2, chunks)), dma((PAIR, 4)), dma((PAIR, 4, chunks))],
        compiler_params=pltpu.CompilerParams(collective_id=1, has_side_effects=True, vmem_limit_bytes=6 * 2**20),
        name="update_gather",
    )(hyper, nrm, g, *state, *tails)


def pack(grads):
    embed, q, k, v, out, gate, up, down, norms, qk = [g[0] for g in grads]

    def rows(a):
        return a.reshape(-1, 8, COLS, 128).transpose(0, 2, 1, 3)

    def grid(a):
        layers, wide, high = a.shape
        return a.transpose(0, 2, 1).reshape(layers, high // 8, 8, COLS, 128).transpose(0, 1, 3, 2, 4)

    tail = jnp.concatenate([norms.reshape(-1), qk.reshape(-1)])
    tail = jnp.pad(tail, (0, TAIL_BLOCKS * BLK - tail.shape[0]))
    return rows(embed), grid(q), grid(k), grid(v), rows(out), grid(gate), grid(up), rows(down), rows(tail.reshape(-1, 4608))


def block_runs(b0, b1):
    cuts = [own_start(r) for r in range(GROUP + 1)]
    out = []
    for r in range(GROUP):
        lo, hi = max(b0, cuts[r]), min(b1, cuts[r + 1])
        if lo < hi:
            out.append((r * OWN + lo - cuts[r], hi - lo))
    return out


def unpack_kernel(o, embed, q, k, v, out, gate, up, down, tail, buf, in_sem, out_sem):
    def rows_out(ref, first):
        def store(slot, count):
            pltpu.make_async_copy(
                buf.at[slot, pl.ds(0, count)], ref.at[pl.ds(first, count)], out_sem.at[slot]).start()
        return store

    def grid_out(ref, layer):
        def store(slot, count):
            def one(rt, z):
                pltpu.make_async_copy(buf.at[slot, :, rt], ref.at[layer, rt], out_sem.at[slot]).start()
                return z
            lax.fori_loop(0, COLS, one, 0)
        return store

    def cols_out(ref, parts):
        high, wide = ref.shape[1], COLS // parts

        def store(slot, count):
            def one(n, z):
                for rt in range(high):
                    pltpu.make_async_copy(
                        buf.at[slot, n, pl.ds(wide * rt, wide)],
                        ref.at[n // parts, rt, pl.ds((n % parts) * wide, wide)], out_sem.at[slot]).start()
                return z
            lax.fori_loop(0, count, one, 0)
        return store

    jobs = []

    def add_rows(ref, b0, b1):
        for lo in range(b0, b1, COLS):
            hi = min(lo + COLS, b1)
            jobs.append((lo, hi - lo, rows_out(ref, lo - b0)))

    e = EDGES
    add_rows(embed, 0, e[1])
    for layer in range(gate.shape[0]):
        jobs.append((e[5] + COLS * layer, COLS, grid_out(gate, layer)))
        jobs.append((e[6] + COLS * layer, COLS, grid_out(up, layer)))
    jobs.append((e[1], e[2] - e[1], cols_out(q, 4)))
    jobs.append((e[2], e[3] - e[2], cols_out(k, 2)))
    jobs.append((e[3], e[4] - e[3], cols_out(v, 2)))
    add_rows(out, e[4], e[5])
    add_rows(down, e[7], e[8])
    add_rows(tail, e[8], e[8] + 4)
    depth = buf.shape[0]

    def load(n):
        b0, count, _ = jobs[n]
        at = 0
        for first, size in block_runs(b0, b0 + count):
            pltpu.make_async_copy(
                o.at[pl.ds(first, size)], buf.at[n % depth, pl.ds(at, size)], in_sem.at[n % depth]).start()
            at += size

    def wait(n, sem):
        view = buf.at[n % depth, pl.ds(0, jobs[n][1])]
        pltpu.make_async_copy(view, view, sem.at[n % depth]).wait()

    lead = depth // 2
    for n in range(len(jobs) + lead):
        if n < len(jobs):
            if n >= depth:
                wait(n - depth, out_sem)
            load(n)
        if n >= lead:
            wait(n - lead, in_sem)
            jobs[n - lead][2]((n - lead) % depth, jobs[n - lead][1])
    for n in range(len(jobs) - depth, len(jobs)):
        wait(n, out_sem)


def run_unpack(o, shapes):
    e, bf16 = EDGES, jnp.bfloat16
    any_spec = pl.BlockSpec(memory_space=pl.ANY)

    def rows(n):
        return (n,) + TILE

    def grid(shape):
        return (shape[0], shape[2] // 8) + TILE
    views = [rows(e[1]), grid(shapes[1]), grid(shapes[2]), grid(shapes[3]), rows(e[5] - e[4]),
             grid(shapes[5]), grid(shapes[6]), rows(e[8] - e[7]), rows(4)]
    dma = pltpu.SemaphoreType.DMA
    depth = 4
    outs = pl.pallas_call(
        unpack_kernel, out_shape=[jax.ShapeDtypeStruct(s, bf16) for s in views],
        in_specs=[any_spec], out_specs=[any_spec] * len(views),
        scratch_shapes=[pltpu.VMEM((depth, COLS) + TILE, bf16), dma((depth,)), dma((depth,))],
        compiler_params=pltpu.CompilerParams(vmem_limit_bytes=12 * 2**20),
        name="unpack",
    )(o)

    def from_rows(a, shape):
        return a.swapaxes(1, 2).reshape(shape)

    def from_grid(a, shape):
        layers, wide, high = shape
        return a.swapaxes(2, 3).reshape(layers, high, wide).swapaxes(1, 2)
    params = [(from_grid if len(a.shape) > 4 else from_rows)(a, s) for a, s in zip(outs[:8], shapes)]
    tail = from_rows(outs[8], (-1,))
    size = math.prod(shapes[8])
    params.append(tail[:size].reshape(shapes[8]))
    params.append(tail[size:size + math.prod(shapes[9])].reshape(shapes[9]))
    return tuple(params)


def solution(mesh):
    group_size = mesh.shape["dp"]
    assert group_size == GROUP

    def local_update(*arrays):
        grads = arrays[:GRAD_COUNT]
        first_part, second_part, master_part, hyper_params = arrays[GRAD_COUNT:]
        state = (first_part, second_part, master_part)
        shapes = [grad_arr.shape[1:] for grad_arr in grads]

        heads = jnp.concatenate([s[:BLK] for s in state])
        heads = lax.ppermute(heads, "dp", [(r + 1, r) for r in range(GROUP - 1)])
        rest = 2 * BLK - (SHARE - 121 * BLK) - BLK
        tails = [jnp.concatenate([s[121 * BLK:], heads[n * BLK:(n + 1) * BLK], jnp.zeros((rest,), s.dtype)])
                 for n, s in enumerate(state)]

        g, nrm = run_reduce(pack(grads))
        *moved, o = run_update(hyper_params, nrm, g, state, tails)
        o, *moved = lax.optimization_barrier([o] + [a[:SHARE] for a in moved])
        return run_unpack(o.reshape((-1,) + TILE), shapes) + tuple(moved)

    in_specs = tuple([P("dp")] * GRAD_COUNT + [P("dp"), P("dp"), P("dp"), P()])
    out_specs = tuple([P()] * GRAD_COUNT + [P("dp"), P("dp"), P("dp")])
    return jax.shard_map(local_update, mesh=mesh, in_specs=in_specs, out_specs=out_specs, check_vma=False)
```

```python
import functools
import math
import jax
import jax.numpy as jnp
from jax import lax
from jax.experimental import pallas as pl
from jax.experimental.pallas import tpu as pltpu
from jax.sharding import PartitionSpec as P

ADAM_STEP = 7
ADAM_EPS = 1e-8
CLIP_EPS = 1e-6
GRAD_COUNT = 10
NORM_COUNT = 2
MESH = pl.DeviceIdType.MESH

GROUP = 8
PAIR = 2
HALVES = range(PAIR)
OTHERS = range(1, GROUP)
STATE = range(3)
ALL = range(4)
BLK = 36864
ROWS = 288
SHARE = 4483776
HALF = 62
COVER = 2 * HALF
CH = 2
CHUNKS = HALF // CH
AHEAD = 3
SLOTS = 8
OWN = 122
OWN_HALF = OWN // 2
GATHERED = 52
LATE = OWN - 2 * GATHERED
EDGES = (0, 250, 274, 286, 298, 322, 538, 754, 970, 976)
TAIL_BLOCKS = 6
TILE = (36, 8, 128)
COLS = 36
NEAR_LAG = 2
FAR_LAG = 4
PART = 2
DECAY_LEN = 970 * BLK


def cover_start(r):
    return (r * SHARE) // BLK


def own_start(r):
    return (r * SHARE + BLK - 1) // BLK


def kind_of(b):
    is_q = (b >= EDGES[1]) & (b < EDGES[2])
    is_kv = (b >= EDGES[2]) & (b < EDGES[4])
    is_gate = (b >= EDGES[5]) & (b < EDGES[7])
    is_row = (b < EDGES[1]) | ((b >= EDGES[4]) & (b < EDGES[5])) | (b >= EDGES[7])
    return is_row, is_gate, is_q, is_kv


def lane_pick(parts, width):
    lane = lax.broadcasted_iota(jnp.int32, parts[0].shape, 1)
    out = parts[0]
    for i in range(1, len(parts)):
        out = jnp.where(lane >= i * width, parts[i], out)
    return out


def roll_to(x, src, dst):
    shift = (dst - src) % 128
    return pltpu.roll(x, shift, 1) if shift else x


def tile_order(kind):
    if kind == "gate":
        return list(range(36))
    if kind == "q":
        return [rt * 9 + ct for ct in range(9) for rt in range(4)]
    return [rt * 18 + ct for ct in range(18) for rt in HALVES]


def pieces(kind):
    out = []
    if kind == "gate":
        for f in range(9):
            for q in range(4):
                k = 4 * f + q
                dd, a = k // 9, k % 9
                out.append(((f, 32, 9), q, (a // 4, dd, 4), a % 4))
    elif kind == "q":
        for ct in range(9):
            for q in range(4):
                out.append(((32 * ct, 32, 1), q, (ct // 4, q, 4), ct % 4))
    else:
        for ct in range(18):
            for q in range(8):
                out.append(((16 * ct, 16, 1), q, (ct // 8, q, 8), ct % 8))
    return out


def width_of(kind):
    return 16 if kind == "kv" else 32


def rows_to_joined(src, dst):
    for i in range(8):
        dst[pl.ds(36 * i, 36), :] = src[:, i, :]


def joined_to_rows(src, emit):
    for t in range(36):
        emit(t, src[pl.ds(t, 8, stride=36), :])


def transposed_to_joined(kind, src, tbuf, dst):
    order = tile_order(kind)
    for j in range(3):
        tiles = [src[t] for t in order[16 * j:16 * j + 16]]
        if len(tiles) < 16:
            tiles.append(jnp.zeros((128 - 8 * len(tiles), 128), jnp.float32))
        tbuf[j] = jnp.concatenate(tiles, axis=0).T
    w = width_of(kind)
    groups = {}
    for drows, dl, srows, sl in pieces(kind):
        groups.setdefault(drows, []).append((dl, srows, sl))
    for (start, count, stride), items in groups.items():
        parts = [None] * (128 // w)
        for dl, (g, s0, sstr), sl in items:
            parts[dl] = roll_to(tbuf[g, pl.ds(s0, count, stride=sstr), :], sl * w, dl * w)
        value = lane_pick(parts, w)
        if stride == 1:
            dst[pl.ds(start, count), :] = value
        else:
            dst[pl.ds(start, count, stride=stride), :] = value


def joined_to_transposed(kind, src, tbuf, emit):
    order = tile_order(kind)
    w = width_of(kind)
    groups = {}
    for drows, dl, srows, sl in pieces(kind):
        groups.setdefault(srows, []).append((sl, drows, dl))
    for (g, s0, sstr), items in groups.items():
        count = items[0][1][1]
        parts = [None] * (128 // w)
        for sl, (start, cnt, stride), dl in items:
            if stride == 1:
                rows = src[pl.ds(start, cnt), :]
            else:
                rows = src[pl.ds(start, cnt, stride=stride), :]
            parts[sl] = roll_to(rows, dl * w, sl * w)
        filler = next(p for p in parts if p is not None)
        parts = [filler if p is None else p for p in parts]
        tbuf[g, pl.ds(s0, count, stride=sstr), :] = lane_pick(parts, w)
    for j in range(3):
        block = tbuf[j].T
        for n, t in enumerate(order[16 * j:16 * j + 16]):
            emit(t, block[8 * n:8 * n + 8, :])


def positions(me):
    y, x, c = me // 4, (me // 2) % 2, me % 2
    xn, yn = 1 - x, 1 - y
    return y, x, c, xn, yn


def dev(y, x, c):
    return (y * 2 + x) * 2 + c


def by_block(b, refs, fn):
    for kind, ref in enumerate(refs):
        first, last = EDGES[kind], EDGES[kind + 1]
        shape = ref.shape

        @pl.when((b >= first) & (b < last))
        def _(ref=ref, shape=shape, n=b - first):
            if len(shape) == 4:
                fn(ref.at[n], 0, COLS)
                return
            high = shape[1]
            wide = COLS // high
            layer, part = n // high, n % high
            if wide == 1:
                fn(ref.at[layer, :, part], 0, COLS)
            else:
                for rt in range(high):
                    fn(ref.at[layer, rt, pl.ds(part * wide, wide)], rt * wide, wide)


def reduce_kernel(e_in, q_in, k_in, v_in, o_in, gate_in, up_in, down_in, tail_in, g_hbm, nrm_ref, r1, r2, ld, ld2, st, sbuf, tbuf, fbuf, acc, nbuf,
                  s1_send, s1_recv, s2_send, s2_recv, ld_sem, g_sem, n_send, n_recv):
    me = lax.axis_index("dp")
    y, x, c, xn, yn = positions(me)
    sources = (e_in, q_in, k_in, v_in, o_in, gate_in, up_in, down_in, tail_in)
    barrier = pltpu.get_barrier_semaphore()
    for o in OTHERS:
        pl.semaphore_signal(barrier, inc=1, device_id=((me + o) % GROUP,), device_id_type=MESH)
    pl.semaphore_wait(barrier, GROUP - 1)

    partner = dev(y, x, 1 - c)
    def targets(h):
        cy, cx = (y, xn) if h == 0 else (yn, x)
        oy, ox = (1 - cy, cx) if h == 0 else (cy, 1 - cx)
        py, px = (1 - y, x) if h == 0 else (y, 1 - x)
        return (
            (partner, 0, (dev(py, px, 1 - c), partner)),
            (dev(cy, cx, 0), 1 + c, (dev(oy, ox, 0), dev(cy, cx, 0))),
            (dev(cy, cx, 1), 1 + c, (dev(oy, ox, 1), dev(cy, cx, 1))),
        )

    def send(h, n, t):
        d, k = t // CHUNKS, t % CHUNKS
        device, slot, dests = targets(h)[n]
        dest = dests[0] * (1 - d) + dests[1] * d
        for j in range(CH):
            at = k * CH + j

            def start(src, tile, tiles):
                pltpu.make_async_remote_copy(
                    src_ref=src, dst_ref=r1.at[h, slot, d, at, pl.ds(tile, tiles)],
                    send_sem=s1_send.at[h, n, t % SLOTS], recv_sem=s1_recv.at[h, slot, t],
                    device_id=(device,), device_id_type=MESH).start()
            by_block(cover_start(dest) + h * HALF + at, sources, start)

    def sent(h, n, t):
        view = ld.at[h, 0]
        pltpu.make_async_copy(view, view, s1_send.at[h, n, t % SLOTS]).wait()

    total_steps = 2 * CHUNKS

    def issue(t):
        @pl.when(t < total_steps)
        def _():
            for n in (1, 2, 0):
                for h in HALVES:
                    @pl.when(t >= SLOTS)
                    def _():
                        sent(h, n, t - SLOTS)
                    send(h, n, t)

    def first_issue(t, carry):
        issue(t)
        return carry

    lax.fori_loop(0, AHEAD, first_issue, 0)

    other = (dev(yn, x, c), dev(y, xn, c))

    def wait_stage1(h, t):
        d, k = t // CHUNKS, t % CHUNKS
        for slot in range(3):
            view = r1.at[h, slot, d, pl.ds(k * CH, CH)]
            pltpu.make_async_copy(view, view, s1_recv.at[h, slot, t]).wait()

    def start_loads(h, t, dest):
        d, k = t // CHUNKS, t % CHUNKS
        for j in range(CH):
            def start(src, tile, tiles):
                pltpu.make_async_copy(
                    src, ld.at[h, 3, j, pl.ds(tile, tiles)], ld_sem.at[h, 3]).start()
            by_block(cover_start(dest) + h * HALF + k * CH + j, sources, start)
        for slot in range(3):
            pltpu.make_async_copy(
                r1.at[h, slot, d, pl.ds(k * CH, CH)], ld.at[h, slot], ld_sem.at[h, slot]).start()

    def wait_loads(h):
        for slot in range(4):
            pltpu.make_async_copy(ld.at[h, slot], ld.at[h, slot], ld_sem.at[h, slot]).wait()

    def partial_sum(h, j, t0):
        rows = [ld[h, s, j, pl.ds(t0, 4)].astype(jnp.float32) for s in range(4)]
        return (rows[3] + rows[0]) + (rows[1] + rows[2])

    def stage2_copy(h, k):
        return pltpu.make_async_remote_copy(
            src_ref=st.at[h, k % SLOTS], dst_ref=r2.at[h, pl.ds(k * CH, CH)],
            send_sem=s2_send.at[h, k % SLOTS], recv_sem=s2_recv.at[h, k],
            device_id=(other[h],), device_id_type=MESH)

    def other_step(k, carry):
        issue(k + AHEAD)
        for h in HALVES:
            wait_stage1(h, k)
            start_loads(h, k, other[h])
        for h in HALVES:
            @pl.when(k >= SLOTS)
            def _():
                stage2_copy(h, k - SLOTS).wait_send()
            wait_loads(h)
            for j in range(CH):
                def add(i, z):
                    st[h, k % SLOTS, j, pl.ds(i * 4, 4)] = partial_sum(h, j, i * 4)
                    return z
                lax.fori_loop(0, 9, add, 0)
            stage2_copy(h, k).start()
        return carry

    lax.fori_loop(0, CHUNKS, other_step, 0)

    acc[...] = jnp.zeros_like(acc)
    first, last = own_start(me), own_start(me + 1)

    def g_copy(h, k):
        row = pl.multiple_of((h * HALF + k * CH) * ROWS, 8)
        return pltpu.make_async_copy(
            fbuf.at[h, k % 2], g_hbm.at[pl.ds(row, CH * ROWS)], g_sem.at[h, k % 2])

    def own_step(k, carry):
        t = k + CHUNKS
        issue(t + AHEAD)
        for h in HALVES:
            wait_stage1(h, t)
            view = r2.at[h, pl.ds(k * CH, CH)]
            pltpu.make_async_copy(view, view, s2_recv.at[h, k]).wait()
            start_loads(h, t, me)
            pltpu.make_async_copy(view, ld2.at[h], ld_sem.at[h, 4]).start()
        for h in HALVES:
            @pl.when(k >= 2)
            def _():
                g_copy(h, k - 2).wait()
            wait_loads(h)
            pltpu.make_async_copy(ld2.at[h], ld2.at[h], ld_sem.at[h, 4]).wait()
            for j in range(CH):
                b = cover_start(me) + h * HALF + k * CH + j
                weight = jnp.where((b >= first) & (b < last), 1.0, 0.0)

                def add(i, z):
                    s = partial_sum(h, j, i * 4) + ld2[h, j, pl.ds(i * 4, 4)]
                    sbuf[pl.ds(i * 4, 4)] = s
                    return z + jnp.sum(s * s, axis=0)
                sq = lax.fori_loop(0, 9, add, jnp.zeros((8, 128), jnp.float32))
                acc[...] += sq * weight
                dst = fbuf.at[h, k % 2, pl.ds(j * ROWS, ROWS)]
                is_row, is_gate, is_q, is_kv = kind_of(b)
                pl.when(is_row)(functools.partial(rows_to_joined, sbuf, dst))
                pl.when(is_gate)(functools.partial(transposed_to_joined, "gate", sbuf, tbuf, dst))
                pl.when(is_q)(functools.partial(transposed_to_joined, "q", sbuf, tbuf, dst))
                pl.when(is_kv)(functools.partial(transposed_to_joined, "kv", sbuf, tbuf, dst))
            g_copy(h, k).start()
        return carry

    lax.fori_loop(0, CHUNKS, own_step, 0)

    nbuf[me] = acc[...]

    def norm_copy(o):
        return pltpu.make_async_remote_copy(
            src_ref=acc, dst_ref=nbuf.at[me], send_sem=n_send.at[o - 1], recv_sem=n_recv.at[me],
            device_id=((me + o) % GROUP,), device_id_type=MESH)

    for o in OTHERS:
        norm_copy(o).start()
    for h in HALVES:
        for k in range(CHUNKS - 2, CHUNKS):
            g_copy(h, k).wait()
        for k in range(CHUNKS - SLOTS, CHUNKS):
            stage2_copy(h, k).wait_send()
        for n in STATE:
            for t in range(total_steps - SLOTS, total_steps):
                sent(h, n, t)
    for o in OTHERS:
        peer = (me + o) % GROUP
        pltpu.make_async_copy(nbuf.at[peer], nbuf.at[peer], n_recv.at[peer]).wait()
    for o in OTHERS:
        norm_copy(o).wait_send()
    total = nbuf[0]
    for i in OTHERS:
        total = total + nbuf[i]
    nrm_ref[...] = total


def run_reduce(sources):
    any_spec = pl.BlockSpec(memory_space=pl.ANY)
    f32, bf16 = jnp.float32, jnp.bfloat16
    tile = TILE
    out_shape = (
        jax.ShapeDtypeStruct((COVER * ROWS, 128), f32),
        jax.ShapeDtypeStruct((8, 128), f32),
        jax.ShapeDtypeStruct((2, 3, 2, HALF) + tile, bf16),
        jax.ShapeDtypeStruct((2, HALF) + tile, f32),
    )
    dma = pltpu.SemaphoreType.DMA
    outs = pl.pallas_call(
        reduce_kernel, out_shape=out_shape, in_specs=[any_spec] * len(sources),
        out_specs=(any_spec, pl.BlockSpec(memory_space=pltpu.VMEM), any_spec, any_spec),
        scratch_shapes=[
            pltpu.VMEM((2, 4, CH) + tile, bf16),
            pltpu.VMEM((2, CH) + tile, f32),
            pltpu.VMEM((2, SLOTS, CH) + tile, f32),
            pltpu.VMEM(tile, f32),
            pltpu.VMEM((3, 128, 128), f32),
            pltpu.VMEM((2, 2, CH * ROWS, 128), f32),
            pltpu.VMEM((8, 128), f32),
            pltpu.VMEM((GROUP, 8, 128), f32),
            dma((PAIR, 3, SLOTS)), dma((PAIR, 3, 2 * CHUNKS)), dma((PAIR, SLOTS)), dma((PAIR, CHUNKS)),
            dma((PAIR, 5)), dma((PAIR, 2)), dma((GROUP - 1,)), dma((GROUP,)),
        ],
        compiler_params=pltpu.CompilerParams(collective_id=0, has_side_effects=True),
        name="reduce_scatter",
    )(*sources)
    return outs[0], outs[1]


def update_kernel(hyper_ref, nrm_ref, g_hbm, m_hbm, v_hbm, p_hbm, mt, vt, pt,
                  m_out, v_out, p_out, o, late, gbuf, pbuf, fbuf, tbuf, cbuf, gin, sin, sout, obuf,
                  in_sem, out_sem, o_sem, f_send, f_recv, s_send, s_recv, p_send, p_recv):
    me = lax.axis_index("dp")
    y, x, c, xn, yn = positions(me)
    partner = dev(y, x, 1 - c)
    near = (dev(yn, x, c), dev(y, xn, c))
    far = dev(yn, xn, c)
    barrier = pltpu.get_barrier_semaphore()
    for device in (partner,) + near:
        pl.semaphore_signal(barrier, inc=1, device_id=(device,), device_id_type=MESH)
    pl.semaphore_wait(barrier, 3)

    lr, b1, b2, wd, max_norm = [hyper_ref[n] for n in range(5)]
    delta = me * SHARE - cover_start(me) * BLK
    rho, odd = delta // 128, me % 2 == 1
    sigma = (own_start(me) * BLK - me * SHARE) // 128
    low, high = pl.ds(0, ROWS), pl.ds(ROWS, ROWS)
    state, tails, outs = (m_hbm, v_hbm, p_hbm), (mt, vt, pt), (m_out, v_out)
    size = 32
    lane = lax.broadcasted_iota(jnp.int32, (size, 128), 1)
    sub = lax.broadcasted_iota(jnp.int32, (size, 128), 0)
    own_lane = (lane < 64) | jnp.logical_not(odd)

    def place(buf, at, count, value):
        @pl.when(odd)
        def _():
            buf[pl.ds(at, count), :] = pltpu.roll(value(), 64, 1)

        @pl.when(jnp.logical_not(odd))
        def _():
            buf[pl.ds(at, count), :] = value()

    def window(buf, row, j):
        at = row + size * j
        return jnp.where(own_lane, buf[pl.ds(at, size), :], buf[pl.ds(at + 1, size), :])

    def flat(i, n, first=0, count=BLK):
        return pl.ds(pl.multiple_of((i % 2 * 3 + n) * BLK + first, 1024), count)

    def span(i):
        return pl.ds(pl.multiple_of(i * BLK, 1024), BLK)

    def g_copy(i, slot):
        rows = pl.ds(pl.multiple_of(i * ROWS, 8), ROWS)
        return pltpu.make_async_copy(g_hbm.at[rows], gin.at[slot], in_sem.at[slot, 3])

    def start_loads(i):
        g_copy(i + 1, i % 2).start()
        for n in STATE:
            @pl.when(i < OWN - 1)
            def _():
                pltpu.make_async_copy(state[n].at[span(i)], sin.at[flat(i, n)], in_sem.at[i % 2, n]).start()

            @pl.when(i >= OWN - 1)
            def _():
                pltpu.make_async_copy(
                    tails[n].at[span(i - OWN + 1)], sin.at[flat(i, n)], in_sem.at[i % 2, n]).start()

    def store_copy(i):
        return pltpu.make_async_copy(
            sout.at[pl.ds(pl.multiple_of(i % 2 * BLK, 1024), BLK)], p_out.at[span(i)], out_sem.at[i % 2])

    def block_start(j):
        @pl.when(j < 2 * GATHERED)
        def _():
            pltpu.make_async_copy(
                obuf.at[j % SLOTS], o.at[me * GATHERED + j // 2, j % 2], o_sem.at[j % SLOTS]).start()

        @pl.when(j >= 2 * GATHERED)
        def _():
            pltpu.make_async_copy(obuf.at[j % SLOTS], late.at[j - 2 * GATHERED], o_sem.at[j % SLOTS]).start()

    def block_wait(j):
        pltpu.make_async_copy(obuf.at[j % SLOTS], late.at[0], o_sem.at[j % SLOTS]).wait()

    def step(i):
        @pl.when(i < OWN)
        def _():
            start_loads(i + 1)
        g_copy(i + 1, i % 2).wait()
        for n in STATE:
            view = sin.at[flat(i, n)]
            pltpu.make_async_copy(view, view, in_sem.at[i % 2, n]).wait()
        pl.when(i >= 2)(lambda: store_copy(i - 2).wait())
        gbuf[low, :] = gbuf[high, :]
        pbuf[low, :] = pbuf[high, :]
        place(gbuf, ROWS, ROWS, lambda: gin[i % 2])
        scale, inv1, inv2 = [cbuf[n, :1] for n in STATE]
        for j in range(ROWS // size):
            first, count = size * 128 * j, size * 128
            h = window(gbuf, rho, j) * scale
            m, v, p = [sin[flat(i, n, first, count)].reshape(size, 128) for n in STATE]
            m1 = b1 * m + (1.0 - b1) * h
            v1 = b2 * v + (1.0 - b2) * (h * h)
            pos = me * SHARE + i * BLK + first + sub * 128 + lane
            decay = jnp.where(pos < DECAY_LEN, wd * p, 0.0)
            u = (m1 * inv1) / (jnp.sqrt(v1 * inv2) + ADAM_EPS) + decay
            p1 = p - lr * u
            place(pbuf, ROWS + size * j, size, lambda: p1)
            sout[pl.ds(pl.multiple_of(i % 2 * BLK + first, 1024), count)] = p1.reshape(count)

            @pl.when(i < OWN)
            def _():
                for n, value in enumerate((m1, v1)):
                    outs[n][pl.ds(pl.multiple_of(i * BLK + first, 1024), count)] = value.reshape(count)

        pl.when(i < OWN)(lambda: store_copy(i).start())

    def finish(i):
        j = i - 1
        for k in range(ROWS // size):
            fbuf[pl.ds(size * k, size), :] = window(pbuf, sigma, k)
        b = own_start(me) + j

        def emit(t, value):
            obuf[j % SLOTS, t] = value.astype(jnp.bfloat16)
        is_row, is_gate, is_q, is_kv = kind_of(b)
        pl.when(is_row)(functools.partial(joined_to_rows, fbuf, emit))
        pl.when(is_gate)(functools.partial(joined_to_transposed, "gate", fbuf, tbuf, emit))
        pl.when(is_q)(functools.partial(joined_to_transposed, "q", fbuf, tbuf, emit))
        pl.when(is_kv)(functools.partial(joined_to_transposed, "kv", fbuf, tbuf, emit))
        block_start(j)

    def view(h, share, q, count):
        return o.at[pl.ds(share * GATHERED + q * PART, count), h]

    def copy(h, share, q, count, send, recv, device):
        span_ = view(h, share, q, count)
        pltpu.make_async_remote_copy(
            src_ref=span_, dst_ref=span_, send_sem=send, recv_sem=recv,
            device_id=(device,), device_id_type=MESH).start()

    def to_partner(h, which, q, count):
        share = (me, near[h], near[1 - h], far)[which]
        copy(h, share, q, count, p_send.at[h, which], p_recv.at[h, which, q], partner)

    def second_hop(h, which, q, count):
        share = (me, near[h])[which]
        copy(h, share, q, count, s_send.at[h, which], s_recv.at[h, which, q], near[1 - h])

    def arrived(h, count, sem):
        span_ = view(h, 0, 0, count)
        pltpu.make_async_copy(span_, span_, sem).wait()

    def stored(q, count):
        for n in range(2 * count):
            block_wait(2 * PART * q + n)

    def send_own(q, count):
        for h in HALVES:
            copy(h, me, q, count, f_send.at[h], f_recv.at[h, q], near[h])
            second_hop(h, 0, q, count)
        for h in HALVES:
            to_partner(h, 0, q, count)

    def forward_near(q, count):
        for h in HALVES:
            arrived(h, count, f_recv.at[h, q])
            second_hop(h, 1, q, count)
            to_partner(h, 1, q, count)
        for h in HALVES:
            arrived(h, count, s_recv.at[h, 0, q])
            to_partner(h, 2, q, count)

    def forward_far(q, count):
        for h in HALVES:
            arrived(h, count, s_recv.at[h, 1, q])
            to_partner(h, 3, q, count)

    one = jnp.ones((8, 128), jnp.float32)

    def power(b):
        square = b * b
        cube = b * square
        return cube * (square * square)

    start_loads(jnp.int32(0))
    norm = jnp.sqrt(jnp.sum(nrm_ref[...], keepdims=True) * (1.0 / 64.0))
    clip = jnp.minimum(1.0, (one * max_norm) / (norm + CLIP_EPS))
    cbuf[0] = clip * 0.125
    cbuf[1] = one / (one * (1.0 - power(b1)))
    cbuf[2] = one / (one * (1.0 - power(b2)))
    g_copy(0, 2).start()
    g_copy(0, 2).wait()
    place(gbuf, ROWS, ROWS, lambda: gin[2])

    whole = (OWN_HALF - 1) // PART
    handed = GATHERED // PART
    step(jnp.int32(0))

    def inner(n, q):
        i = 2 * PART * q + n + 1
        step(i)
        finish(i)

        @pl.when((n == 0) & (q >= 1))
        def _():
            stored(q - 1, PART)
            pl.when(q <= handed)(lambda: send_own(q - 1, PART))
        return q

    def outer(q, carry):
        lax.fori_loop(0, 2 * PART, inner, q)
        pl.when((q >= NEAR_LAG) & (q - NEAR_LAG < handed))(lambda: forward_near(q - NEAR_LAG, PART))
        pl.when((q >= FAR_LAG) & (q - FAR_LAG < handed))(lambda: forward_far(q - FAR_LAG, PART))
        return carry

    lax.fori_loop(0, whole, outer, 0)
    stored(whole - 1, PART)

    def last(i, carry):
        step(i)
        finish(i)
        return carry

    lax.fori_loop(OWN - 1, OWN + 1, last, 0)
    stored(whole, 1)

    def rest(fn, first):
        def body(q, carry):
            fn(q, PART)
            return carry
        lax.fori_loop(min(first, handed), handed, body, 0)
    rest(forward_near, whole - NEAR_LAG)
    rest(forward_far, whole - FAR_LAG)

    store_copy(OWN - 1).wait()

    def from_partner(q, count):
        for h in HALVES:
            for which in ALL:
                arrived(h, count, p_recv.at[h, which, q])
    rest(from_partner, 0)
    for h in HALVES:
        arrived(h, GATHERED, f_send.at[h])
        for which in HALVES:
            arrived(h, GATHERED, s_send.at[h, which])
        for which in ALL:
            arrived(h, GATHERED, p_send.at[h, which])


def run_update(hyper, nrm, g, state, tails):
    f32, bf16, dma = jnp.float32, jnp.bfloat16, pltpu.SemaphoreType.DMA
    any_spec = pl.BlockSpec(memory_space=pl.ANY)
    chunks = GATHERED // PART
    rows = pltpu.VMEM((2 * ROWS + 8, 128), f32)
    flat = pltpu.VMEM((6 * BLK,), f32)
    return pl.pallas_call(
        update_kernel,
        in_specs=[pl.BlockSpec(memory_space=pltpu.SMEM), pl.BlockSpec(memory_space=pltpu.VMEM)] + [any_spec] * 7,
        out_specs=[pl.BlockSpec(memory_space=pltpu.VMEM)] * PAIR + [any_spec] * STATE[-1] + [any_spec],
        out_shape=[pltpu.VMEM((OWN * BLK,), f32)] * PAIR + [jax.ShapeDtypeStruct((OWN * BLK,), f32)]
        + [jax.ShapeDtypeStruct(n + TILE, bf16) for n in ((GROUP * GATHERED, 2), (LATE,))],
        scratch_shapes=[
            rows, rows, pltpu.VMEM((ROWS, 128), f32), pltpu.VMEM((3, 128, 128), f32),
            pltpu.VMEM((3, 8, 128), f32), pltpu.VMEM((3, ROWS, 128), f32), flat, pltpu.VMEM((PAIR * BLK,), f32),
            pltpu.VMEM((SLOTS,) + TILE, bf16),
            dma((3, 4)), dma((PAIR,)), dma((SLOTS,)), dma((PAIR,)), dma((PAIR, chunks)), dma((PAIR, 2)),
            dma((PAIR, 2, chunks)), dma((PAIR, 4)), dma((PAIR, 4, chunks))],
        compiler_params=pltpu.CompilerParams(collective_id=1, has_side_effects=True, vmem_limit_bytes=6 * 2**20),
        name="update_gather",
    )(hyper, nrm, g, *state, *tails)


def pack(grads):
    embed, q, k, v, out, gate, up, down, norms, qk = [g[0] for g in grads]

    def rows(a):
        return a.reshape(-1, 8, COLS, 128).transpose(0, 2, 1, 3)

    def grid(a):
        layers, wide, high = a.shape
        return a.transpose(0, 2, 1).reshape(layers, high // 8, 8, COLS, 128).transpose(0, 1, 3, 2, 4)

    tail = jnp.concatenate([norms.reshape(-1), qk.reshape(-1)])
    tail = jnp.pad(tail, (0, TAIL_BLOCKS * BLK - tail.shape[0]))
    return rows(embed), grid(q), grid(k), grid(v), rows(out), grid(gate), grid(up), rows(down), rows(tail.reshape(-1, 4608))


def block_runs(b0, b1):
    out = []
    for r in range(GROUP):
        start = own_start(r)
        lo, hi = max(b0, start), min(b1, own_start(r + 1), start + 2 * GATHERED)
        if lo < hi:
            out.append((r * 2 * GATHERED + lo - start, lo - b0, hi - lo))
    return out


def is_rows(kind):
    return kind in (0, 4, 7, 8)


def unpack_kernel(kinds, o, *refs):
    outs, (buf, in_sem, out_sem) = refs[:len(kinds)], refs[len(kinds):]

    def rows_out(ref, first):
        def store(slot, count):
            pltpu.make_async_copy(
                buf.at[slot, pl.ds(0, count)], ref.at[pl.ds(first, count)], out_sem.at[slot]).start()
        return store

    def grid_out(ref, layer):
        def store(slot, count):
            def one(rt, z):
                pltpu.make_async_copy(buf.at[slot, :, rt], ref.at[layer, rt], out_sem.at[slot]).start()
                return z
            lax.fori_loop(0, COLS, one, 0)
        return store

    def cols_out(ref):
        high = ref.shape[1]
        wide = COLS // high

        def store(slot, count):
            def one(n, z):
                for rt in range(high):
                    pltpu.make_async_copy(
                        buf.at[slot, n, pl.ds(wide * rt, wide)],
                        ref.at[n // high, rt, pl.ds((n % high) * wide, wide)], out_sem.at[slot]).start()
                return z
            lax.fori_loop(0, count, one, 0)
        return store

    jobs = []
    for kind, ref in zip(kinds, outs):
        first = EDGES[kind]
        if is_rows(kind):
            count = ref.shape[0]
            for lo in range(0, count, COLS):
                jobs.append((first + lo, min(COLS, count - lo), rows_out(ref, lo)))
        elif ref.shape[1] == COLS:
            for layer in range(ref.shape[0]):
                jobs.append((first + COLS * layer, COLS, grid_out(ref, layer)))
        else:
            jobs.append((first, EDGES[kind + 1] - first, cols_out(ref)))
    depth = buf.shape[0]

    def load(n):
        b0, count, _ = jobs[n]
        for first, at, size in block_runs(b0, b0 + count):
            pltpu.make_async_copy(
                o.at[pl.ds(first, size)], buf.at[n % depth, pl.ds(at, size)], in_sem.at[n % depth]).start()

    def wait(n, count, sem):
        if count:
            view = buf.at[n % depth, pl.ds(0, count)]
            pltpu.make_async_copy(view, view, sem.at[n % depth]).wait()

    def loaded(n):
        b0, count, _ = jobs[n]
        return sum(size for _, _, size in block_runs(b0, b0 + count))

    lead = depth // 2
    for n in range(len(jobs) + lead):
        if n < len(jobs):
            if n >= depth:
                wait(n - depth, jobs[n - depth][1], out_sem)
            load(n)
        if n >= lead:
            wait(n - lead, loaded(n - lead), in_sem)
            jobs[n - lead][2]((n - lead) % depth, jobs[n - lead][1])
    for n in range(len(jobs) - depth, len(jobs)):
        wait(n, jobs[n][1], out_sem)


def late_kernel(*refs):
    count = len(EDGES) - 1
    late, outs = refs[:GROUP], refs[GROUP + count:GROUP + 2 * count]
    buf, in_sem, out_sem = refs[GROUP + 2 * count:]
    me = lax.axis_index("dp")
    y, x, c, _, _ = positions(me)
    for k in range(GROUP):
        pltpu.make_async_copy(late[k], buf.at[k], in_sem).start()
    pltpu.make_async_copy(buf, buf, in_sem).wait()

    def differs(bit, mine):
        return 1 - mine if bit else mine

    for r in range(GROUP):
        ry, rx, rc, _, _ = positions(r)
        k = dev(differs(ry, y), differs(rx, x), differs(rc, c))
        start, end = own_start(r) + 2 * GATHERED, own_start(r + 1)
        for kind, ref in enumerate(outs):
            lo, hi = max(start, EDGES[kind]), min(end, EDGES[kind + 1])
            if lo >= hi:
                continue
            if is_rows(kind):
                pltpu.make_async_copy(
                    buf.at[k, pl.ds(lo - start, hi - lo)], ref.at[pl.ds(lo - EDGES[kind], hi - lo)],
                    out_sem).start()
                continue
            assert ref.shape[1] == COLS
            for layer in range(ref.shape[0]):
                base = EDGES[kind] + COLS * layer
                at, to = max(lo, base), min(hi, base + COLS)
                if at < to:
                    def one(rt, z, ref=ref, layer=layer, k=k, n=at - start, col=at - base, tiles=to - at):
                        pltpu.make_async_copy(
                            buf.at[k, pl.ds(n, tiles), rt], ref.at[layer, rt, pl.ds(col, tiles)],
                            out_sem).start()
                        return z
                    lax.fori_loop(0, COLS, one, 0)
    for r in range(GROUP):
        view = buf.at[r, pl.ds(0, own_start(r + 1) - own_start(r) - 2 * GATHERED)]
        pltpu.make_async_copy(view, view, out_sem).wait()


def out_views(shapes):
    views = []
    for kind in range(len(EDGES) - 1):
        if is_rows(kind):
            views.append((EDGES[kind + 1] - EDGES[kind],) + TILE)
        else:
            views.append((shapes[kind][0], shapes[kind][2] // 8) + TILE)
    return views


def run_unpack(o, kinds, views):
    bf16, dma, depth = jnp.bfloat16, pltpu.SemaphoreType.DMA, 4
    any_spec = pl.BlockSpec(memory_space=pl.ANY)
    size = sum(math.prod(views[kind]) for kind in kinds)
    return pl.pallas_call(
        functools.partial(unpack_kernel, kinds),
        out_shape=[jax.ShapeDtypeStruct(views[kind], bf16) for kind in kinds],
        in_specs=[any_spec], out_specs=[any_spec] * len(kinds),
        scratch_shapes=[pltpu.VMEM((depth, COLS) + TILE, bf16), dma((depth,)), dma((depth,))],
        cost_estimate=pl.CostEstimate(flops=size * 1000, bytes_accessed=size * 4, transcendentals=0),
        compiler_params=pltpu.CompilerParams(vmem_limit_bytes=12 * 2**20),
        name="unpack",
    )(o)


def run_late(late, params):
    bf16, dma, count = jnp.bfloat16, pltpu.SemaphoreType.DMA, len(params)
    any_spec = pl.BlockSpec(memory_space=pl.ANY)
    return pl.pallas_call(
        late_kernel, out_shape=[jax.ShapeDtypeStruct(a.shape, bf16) for a in params],
        in_specs=[any_spec] * (GROUP + count), out_specs=[any_spec] * count,
        input_output_aliases={GROUP + n: n for n in range(count)},
        scratch_shapes=[pltpu.VMEM((GROUP, LATE) + TILE, bf16), dma, dma],
        compiler_params=pltpu.CompilerParams(vmem_limit_bytes=12 * 2**20),
        name="unpack_late",
    )(*late, *params)


def to_shapes(outs, shapes):
    def from_rows(a, shape):
        return a.swapaxes(1, 2).reshape(shape)

    def from_grid(a, shape):
        layers, wide, high = shape
        return a.swapaxes(2, 3).reshape(layers, high, wide).swapaxes(1, 2)
    params = [(from_grid if len(a.shape) > 4 else from_rows)(a, s) for a, s in zip(outs[:8], shapes)]
    tail = from_rows(outs[8], (-1,))
    size = math.prod(shapes[8])
    params.append(tail[:size].reshape(shapes[8]))
    params.append(tail[size:size + math.prod(shapes[9])].reshape(shapes[9]))
    return tuple(params)


def swap(a, bit):
    return lax.ppermute(a, "dp", [(r, r ^ bit) for r in range(GROUP)])


def solution(mesh):
    group_size = mesh.shape["dp"]
    assert group_size == GROUP

    def local_update(*arrays):
        grads = arrays[:GRAD_COUNT]
        first_part, second_part, master_part, hyper_params = arrays[GRAD_COUNT:]
        state = (first_part, second_part, master_part)
        shapes = [grad_arr.shape[1:] for grad_arr in grads]

        heads = jnp.concatenate([s[:BLK] for s in state])
        heads = lax.ppermute(heads, "dp", [(r + 1, r) for r in range(GROUP - 1)])
        rest = 2 * BLK - (SHARE - 121 * BLK) - BLK
        tails = [jnp.concatenate([s[121 * BLK:], heads[n * BLK:(n + 1) * BLK], jnp.zeros((rest,), s.dtype)])
                 for n, s in enumerate(state)]

        g, nrm = run_reduce(pack(grads))
        *moved, o, own = run_update(hyper_params, nrm, g, state, tails)
        own, moved[0] = lax.optimization_barrier((own, moved[0][:SHARE]))
        near = [swap(own, bit) for bit in (2, 4, 6)]
        first = swap(own, 1)
        o, *moved = lax.optimization_barrier([o, moved[0]] + [a[:SHARE] for a in moved[1:]])
        o = o.reshape((-1,) + TILE)
        views = out_views(shapes)
        early_kinds, other_kinds = (0, 4, 7, 5), (1, 2, 3, 6, 8)
        early = run_unpack(o, early_kinds, views)
        o, near, early = lax.optimization_barrier((o, near, early))
        cross = [swap(a, 1) for a in near]
        other = run_unpack(o, other_kinds, views)
        cross, other = lax.optimization_barrier((cross, other))
        found = dict(zip(early_kinds + other_kinds, list(early) + list(other)))
        late = [own, first]
        for a, b in zip(near, cross):
            late += [a, b]
        outs = run_late(late, [found[kind] for kind in range(len(views))])
        return to_shapes(outs, shapes) + tuple(moved)

    in_specs = tuple([P("dp")] * GRAD_COUNT + [P("dp"), P("dp"), P("dp"), P()])
    out_specs = tuple([P()] * GRAD_COUNT + [P("dp"), P("dp"), P("dp")])
    return jax.shard_map(local_update, mesh=mesh, in_specs=in_specs, out_specs=out_specs, check_vma=False)
```

```python
import functools
import math
import jax
import jax.numpy as jnp
from jax import lax
from jax.experimental import pallas as pl
from jax.experimental.pallas import tpu as pltpu
from jax.sharding import PartitionSpec as P

ADAM_STEP = 7
ADAM_EPS = 1e-8
CLIP_EPS = 1e-6
GRAD_COUNT = 10
NORM_COUNT = 2
MESH = pl.DeviceIdType.MESH

GROUP = 8
PAIR = 2
HALVES = range(PAIR)
OTHERS = range(1, GROUP)
STATE = range(3)
ALL = range(4)
BLK = 36864
ROWS = 288
SHARE = 4483776
HALF = 62
COVER = 2 * HALF
CH = 2
CHUNKS = HALF // CH
AHEAD = 4
SLOTS = 8
OWN = 122
OWN_HALF = OWN // 2
GATHERED = 52
LATE = OWN - 2 * GATHERED
EDGES = (0, 250, 274, 286, 298, 322, 538, 754, 970, 976)
TAIL_BLOCKS = 6
TILE = (36, 8, 128)
COLS = 36
NEAR_LAG = 5
FAR_LAG = 9
PART = 2
DECAY_LEN = 970 * BLK


def cover_start(r):
    return (r * SHARE) // BLK


def own_start(r):
    return (r * SHARE + BLK - 1) // BLK


def kind_of(b):
    is_q = (b >= EDGES[1]) & (b < EDGES[2])
    is_kv = (b >= EDGES[2]) & (b < EDGES[4])
    is_gate = (b >= EDGES[5]) & (b < EDGES[7])
    is_row = (b < EDGES[1]) | ((b >= EDGES[4]) & (b < EDGES[5])) | (b >= EDGES[7])
    return is_row, is_gate, is_q, is_kv


def lane_pick(parts, width):
    lane = lax.broadcasted_iota(jnp.int32, parts[0].shape, 1)
    out = parts[0]
    for i in range(1, len(parts)):
        out = jnp.where(lane >= i * width, parts[i], out)
    return out


def roll_to(x, src, dst):
    shift = (dst - src) % 128
    return pltpu.roll(x, shift, 1) if shift else x


def tile_order(kind):
    if kind == "gate":
        return list(range(36))
    if kind == "q":
        return [rt * 9 + ct for ct in range(9) for rt in range(4)]
    return [rt * 18 + ct for ct in range(18) for rt in HALVES]


def pieces(kind):
    out = []
    if kind == "gate":
        for f in range(9):
            for q in range(4):
                k = 4 * f + q
                dd, a = k // 9, k % 9
                out.append(((f, 32, 9), q, (a // 4, dd, 4), a % 4))
    elif kind == "q":
        for ct in range(9):
            for q in range(4):
                out.append(((32 * ct, 32, 1), q, (ct // 4, q, 4), ct % 4))
    else:
        for ct in range(18):
            for q in range(8):
                out.append(((16 * ct, 16, 1), q, (ct // 8, q, 8), ct % 8))
    return out


def width_of(kind):
    return 16 if kind == "kv" else 32


def rows_to_joined(src, dst):
    for i in range(8):
        dst[pl.ds(36 * i, 36), :] = src[:, i, :]


def joined_to_rows(src, emit):
    for t in range(36):
        emit(t, src[pl.ds(t, 8, stride=36), :])


def transposed_to_joined(kind, src, tbuf, dst):
    order = tile_order(kind)
    for j in range(3):
        tiles = [src[t] for t in order[16 * j:16 * j + 16]]
        if len(tiles) < 16:
            tiles.append(jnp.zeros((128 - 8 * len(tiles), 128), jnp.float32))
        tbuf[j] = jnp.concatenate(tiles, axis=0).T
    w = width_of(kind)
    groups = {}
    for drows, dl, srows, sl in pieces(kind):
        groups.setdefault(drows, []).append((dl, srows, sl))
    for (start, count, stride), items in groups.items():
        parts = [None] * (128 // w)
        for dl, (g, s0, sstr), sl in items:
            parts[dl] = roll_to(tbuf[g, pl.ds(s0, count, stride=sstr), :], sl * w, dl * w)
        value = lane_pick(parts, w)
        if stride == 1:
            dst[pl.ds(start, count), :] = value
        else:
            dst[pl.ds(start, count, stride=stride), :] = value


def joined_to_transposed(kind, src, tbuf, emit):
    order = tile_order(kind)
    w = width_of(kind)
    groups = {}
    for drows, dl, srows, sl in pieces(kind):
        groups.setdefault(srows, []).append((sl, drows, dl))
    for (g, s0, sstr), items in groups.items():
        count = items[0][1][1]
        parts = [None] * (128 // w)
        for sl, (start, cnt, stride), dl in items:
            if stride == 1:
                rows = src[pl.ds(start, cnt), :]
            else:
                rows = src[pl.ds(start, cnt, stride=stride), :]
            parts[sl] = roll_to(rows, dl * w, sl * w)
        filler = next(p for p in parts if p is not None)
        parts = [filler if p is None else p for p in parts]
        tbuf[g, pl.ds(s0, count, stride=sstr), :] = lane_pick(parts, w)
    for j in range(3):
        block = tbuf[j].T
        for n, t in enumerate(order[16 * j:16 * j + 16]):
            emit(t, block[8 * n:8 * n + 8, :])


def positions(me):
    y, x, c = me // 4, (me // 2) % 2, me % 2
    xn, yn = 1 - x, 1 - y
    return y, x, c, xn, yn


def dev(y, x, c):
    return (y * 2 + x) * 2 + c


def by_block(b, refs, fn):
    for kind, ref in enumerate(refs):
        first, last = EDGES[kind], EDGES[kind + 1]
        shape = ref.shape

        @pl.when((b >= first) & (b < last))
        def _(ref=ref, shape=shape, n=b - first):
            if len(shape) == 4:
                fn(ref.at[n], 0, COLS)
                return
            high = shape[1]
            wide = COLS // high
            layer, part = n // high, n % high
            if wide == 1:
                fn(ref.at[layer, :, part], 0, COLS)
            else:
                for rt in range(high):
                    fn(ref.at[layer, rt, pl.ds(part * wide, wide)], rt * wide, wide)


def reduce_kernel(e_in, q_in, k_in, v_in, o_in, gate_in, up_in, down_in, tail_in, g_hbm, nrm_ref, r1, r2, ld, ld2, st, sbuf, tbuf, fbuf, acc, nbuf,
                  s1_send, s1_recv, s2_send, s2_recv, ld_sem, g_sem, n_send, n_recv):
    me = lax.axis_index("dp")
    y, x, c, xn, yn = positions(me)
    sources = (e_in, q_in, k_in, v_in, o_in, gate_in, up_in, down_in, tail_in)
    barrier = pltpu.get_barrier_semaphore()
    for o in OTHERS:
        pl.semaphore_signal(barrier, inc=1, device_id=((me + o) % GROUP,), device_id_type=MESH)
    pl.semaphore_wait(barrier, GROUP - 1)

    partner = dev(y, x, 1 - c)
    def targets(h):
        cy, cx = (y, xn) if h == 0 else (yn, x)
        oy, ox = (1 - cy, cx) if h == 0 else (cy, 1 - cx)
        py, px = (1 - y, x) if h == 0 else (y, 1 - x)
        return (
            (partner, 0, (dev(py, px, 1 - c), partner)),
            (dev(cy, cx, 0), 1 + c, (dev(oy, ox, 0), dev(cy, cx, 0))),
            (dev(cy, cx, 1), 1 + c, (dev(oy, ox, 1), dev(cy, cx, 1))),
        )

    def send(h, n, t):
        d, k = t // CHUNKS, t % CHUNKS
        device, slot, dests = targets(h)[n]
        dest = dests[0] * (1 - d) + dests[1] * d
        for j in range(CH):
            at = k * CH + j

            def start(src, tile, tiles):
                pltpu.make_async_remote_copy(
                    src_ref=src, dst_ref=r1.at[h, slot, d, at, pl.ds(tile, tiles)],
                    send_sem=s1_send.at[h, n, t % SLOTS], recv_sem=s1_recv.at[h, slot, t],
                    device_id=(device,), device_id_type=MESH).start()
            by_block(cover_start(dest) + h * HALF + at, sources, start)

    def sent(h, n, t):
        view = ld.at[h, 0]
        pltpu.make_async_copy(view, view, s1_send.at[h, n, t % SLOTS]).wait()

    total_steps = 2 * CHUNKS

    def issue(t):
        @pl.when(t < total_steps)
        def _():
            for n in (1, 2, 0):
                for h in HALVES:
                    @pl.when(t >= SLOTS)
                    def _():
                        sent(h, n, t - SLOTS)
                    send(h, n, t)

    def first_issue(t, carry):
        issue(t)
        return carry

    lax.fori_loop(0, AHEAD, first_issue, 0)

    other = (dev(yn, x, c), dev(y, xn, c))

    def wait_stage1(h, t):
        d, k = t // CHUNKS, t % CHUNKS
        for slot in range(3):
            view = r1.at[h, slot, d, pl.ds(k * CH, CH)]
            pltpu.make_async_copy(view, view, s1_recv.at[h, slot, t]).wait()

    def start_loads(h, t, dest):
        d, k = t // CHUNKS, t % CHUNKS
        for j in range(CH):
            def start(src, tile, tiles):
                pltpu.make_async_copy(
                    src, ld.at[h, 3, j, pl.ds(tile, tiles)], ld_sem.at[h, 3]).start()
            by_block(cover_start(dest) + h * HALF + k * CH + j, sources, start)
        for slot in range(3):
            pltpu.make_async_copy(
                r1.at[h, slot, d, pl.ds(k * CH, CH)], ld.at[h, slot], ld_sem.at[h, slot]).start()

    def wait_loads(h):
        for slot in range(4):
            pltpu.make_async_copy(ld.at[h, slot], ld.at[h, slot], ld_sem.at[h, slot]).wait()

    def partial_sum(h, j, t0):
        rows = [ld[h, s, j, pl.ds(t0, 4)].astype(jnp.float32) for s in range(4)]
        return (rows[3] + rows[0]) + (rows[1] + rows[2])

    def stage2_copy(h, k):
        return pltpu.make_async_remote_copy(
            src_ref=st.at[h, k % SLOTS], dst_ref=r2.at[h, pl.ds(k * CH, CH)],
            send_sem=s2_send.at[h, k % SLOTS], recv_sem=s2_recv.at[h, k],
            device_id=(other[h],), device_id_type=MESH)

    def other_step(k, carry):
        issue(k + AHEAD)
        for h in HALVES:
            wait_stage1(h, k)
            start_loads(h, k, other[h])
        for h in HALVES:
            @pl.when(k >= SLOTS)
            def _():
                stage2_copy(h, k - SLOTS).wait_send()
            wait_loads(h)
            for j in range(CH):
                def add(i, z):
                    st[h, k % SLOTS, j, pl.ds(i * 4, 4)] = partial_sum(h, j, i * 4)
                    return z
                lax.fori_loop(0, 9, add, 0)
            stage2_copy(h, k).start()
        return carry

    lax.fori_loop(0, CHUNKS, other_step, 0)

    acc[...] = jnp.zeros_like(acc)
    first, last = own_start(me), own_start(me + 1)

    def g_copy(h, k):
        row = pl.multiple_of((h * HALF + k * CH) * ROWS, 8)
        return pltpu.make_async_copy(
            fbuf.at[h, k % 2], g_hbm.at[pl.ds(row, CH * ROWS)], g_sem.at[h, k % 2])

    def own_step(k, carry):
        t = k + CHUNKS
        issue(t + AHEAD)
        for h in HALVES:
            wait_stage1(h, t)
            view = r2.at[h, pl.ds(k * CH, CH)]
            pltpu.make_async_copy(view, view, s2_recv.at[h, k]).wait()
            start_loads(h, t, me)
            pltpu.make_async_copy(view, ld2.at[h], ld_sem.at[h, 4]).start()
        for h in HALVES:
            @pl.when(k >= 2)
            def _():
                g_copy(h, k - 2).wait()
            wait_loads(h)
            pltpu.make_async_copy(ld2.at[h], ld2.at[h], ld_sem.at[h, 4]).wait()
            for j in range(CH):
                b = cover_start(me) + h * HALF + k * CH + j
                weight = jnp.where((b >= first) & (b < last), 1.0, 0.0)

                def add(i, z):
                    s = partial_sum(h, j, i * 4) + ld2[h, j, pl.ds(i * 4, 4)]
                    sbuf[pl.ds(i * 4, 4)] = s
                    return z + jnp.sum(s * s, axis=0)
                sq = lax.fori_loop(0, 9, add, jnp.zeros((8, 128), jnp.float32))
                acc[...] += sq * weight
                dst = fbuf.at[h, k % 2, pl.ds(j * ROWS, ROWS)]
                is_row, is_gate, is_q, is_kv = kind_of(b)
                pl.when(is_row)(functools.partial(rows_to_joined, sbuf, dst))
                pl.when(is_gate)(functools.partial(transposed_to_joined, "gate", sbuf, tbuf, dst))
                pl.when(is_q)(functools.partial(transposed_to_joined, "q", sbuf, tbuf, dst))
                pl.when(is_kv)(functools.partial(transposed_to_joined, "kv", sbuf, tbuf, dst))
            g_copy(h, k).start()
        return carry

    lax.fori_loop(0, CHUNKS, own_step, 0)

    nbuf[me] = acc[...]

    def norm_copy(o):
        return pltpu.make_async_remote_copy(
            src_ref=acc, dst_ref=nbuf.at[me], send_sem=n_send.at[o - 1], recv_sem=n_recv.at[me],
            device_id=((me + o) % GROUP,), device_id_type=MESH)

    for o in OTHERS:
        norm_copy(o).start()
    for h in HALVES:
        for k in range(CHUNKS - 2, CHUNKS):
            g_copy(h, k).wait()
        for k in range(CHUNKS - SLOTS, CHUNKS):
            stage2_copy(h, k).wait_send()
        for n in STATE:
            for t in range(total_steps - SLOTS, total_steps):
                sent(h, n, t)
    for o in OTHERS:
        peer = (me + o) % GROUP
        pltpu.make_async_copy(nbuf.at[peer], nbuf.at[peer], n_recv.at[peer]).wait()
    for o in OTHERS:
        norm_copy(o).wait_send()
    total = nbuf[0]
    for i in OTHERS:
        total = total + nbuf[i]
    nrm_ref[...] = total


def run_reduce(sources):
    any_spec = pl.BlockSpec(memory_space=pl.ANY)
    f32, bf16 = jnp.float32, jnp.bfloat16
    tile = TILE
    out_shape = (
        jax.ShapeDtypeStruct((COVER * ROWS, 128), f32),
        jax.ShapeDtypeStruct((8, 128), f32),
        jax.ShapeDtypeStruct((2, 3, 2, HALF) + tile, bf16),
        jax.ShapeDtypeStruct((2, HALF) + tile, f32),
    )
    dma = pltpu.SemaphoreType.DMA
    outs = pl.pallas_call(
        reduce_kernel, out_shape=out_shape, in_specs=[any_spec] * len(sources),
        out_specs=(any_spec, pl.BlockSpec(memory_space=pltpu.VMEM), any_spec, any_spec),
        scratch_shapes=[
            pltpu.VMEM((2, 4, CH) + tile, bf16),
            pltpu.VMEM((2, CH) + tile, f32),
            pltpu.VMEM((2, SLOTS, CH) + tile, f32),
            pltpu.VMEM(tile, f32),
            pltpu.VMEM((3, 128, 128), f32),
            pltpu.VMEM((2, 2, CH * ROWS, 128), f32),
            pltpu.VMEM((8, 128), f32),
            pltpu.VMEM((GROUP, 8, 128), f32),
            dma((PAIR, 3, SLOTS)), dma((PAIR, 3, 2 * CHUNKS)), dma((PAIR, SLOTS)), dma((PAIR, CHUNKS)),
            dma((PAIR, 5)), dma((PAIR, 2)), dma((GROUP - 1,)), dma((GROUP,)),
        ],
        compiler_params=pltpu.CompilerParams(collective_id=0, has_side_effects=True),
        name="reduce_scatter",
    )(*sources)
    return outs[0], outs[1]


def update_kernel(hyper_ref, nrm_ref, g_hbm, m_hbm, v_hbm, p_hbm, mt, vt, pt,
                  m_out, v_out, p_out, o, late, gbuf, pbuf, fbuf, tbuf, cbuf, gin, sin, sout, obuf,
                  in_sem, out_sem, o_sem, f_send, f_recv, s_send, s_recv, p_send, p_recv):
    me = lax.axis_index("dp")
    y, x, c, xn, yn = positions(me)
    partner = dev(y, x, 1 - c)
    near = (dev(yn, x, c), dev(y, xn, c))
    far = dev(yn, xn, c)
    barrier = pltpu.get_barrier_semaphore()
    for device in (partner,) + near:
        pl.semaphore_signal(barrier, inc=1, device_id=(device,), device_id_type=MESH)
    pl.semaphore_wait(barrier, 3)

    lr, b1, b2, wd, max_norm = [hyper_ref[n] for n in range(5)]
    delta = me * SHARE - cover_start(me) * BLK
    rho, odd = delta // 128, me % 2 == 1
    sigma = (own_start(me) * BLK - me * SHARE) // 128
    low, high = pl.ds(0, ROWS), pl.ds(ROWS, ROWS)
    state, tails, outs = (m_hbm, v_hbm, p_hbm), (mt, vt, pt), (m_out, v_out)
    size = 32
    lane = lax.broadcasted_iota(jnp.int32, (size, 128), 1)
    sub = lax.broadcasted_iota(jnp.int32, (size, 128), 0)
    own_lane = (lane < 64) | jnp.logical_not(odd)

    def place(buf, at, count, value):
        @pl.when(odd)
        def _():
            buf[pl.ds(at, count), :] = pltpu.roll(value(), 64, 1)

        @pl.when(jnp.logical_not(odd))
        def _():
            buf[pl.ds(at, count), :] = value()

    def window(buf, row, j):
        at = row + size * j
        return jnp.where(own_lane, buf[pl.ds(at, size), :], buf[pl.ds(at + 1, size), :])

    def flat(i, n, first=0, count=BLK):
        return pl.ds(pl.multiple_of((i % 2 * 3 + n) * BLK + first, 1024), count)

    def span(i):
        return pl.ds(pl.multiple_of(i * BLK, 1024), BLK)

    def g_copy(i, slot):
        rows = pl.ds(pl.multiple_of(i * ROWS, 8), ROWS)
        return pltpu.make_async_copy(g_hbm.at[rows], gin.at[slot], in_sem.at[slot, 3])

    def start_loads(i):
        g_copy(i + 1, i % 2).start()
        for n in STATE:
            @pl.when(i < OWN - 1)
            def _():
                pltpu.make_async_copy(state[n].at[span(i)], sin.at[flat(i, n)], in_sem.at[i % 2, n]).start()

            @pl.when(i >= OWN - 1)
            def _():
                pltpu.make_async_copy(
                    tails[n].at[span(i - OWN + 1)], sin.at[flat(i, n)], in_sem.at[i % 2, n]).start()

    def store_copy(i):
        return pltpu.make_async_copy(
            sout.at[pl.ds(pl.multiple_of(i % 2 * BLK, 1024), BLK)], p_out.at[span(i)], out_sem.at[i % 2])

    def block_start(j):
        @pl.when(j < 2 * GATHERED)
        def _():
            pltpu.make_async_copy(
                obuf.at[j % SLOTS], o.at[me * GATHERED + j // 2, j % 2], o_sem.at[j % SLOTS]).start()

        @pl.when(j >= 2 * GATHERED)
        def _():
            pltpu.make_async_copy(obuf.at[j % SLOTS], late.at[j - 2 * GATHERED], o_sem.at[j % SLOTS]).start()

    def block_wait(j):
        pltpu.make_async_copy(obuf.at[j % SLOTS], late.at[0], o_sem.at[j % SLOTS]).wait()

    def step(i):
        @pl.when(i < OWN)
        def _():
            start_loads(i + 1)
        g_copy(i + 1, i % 2).wait()
        for n in STATE:
            view = sin.at[flat(i, n)]
            pltpu.make_async_copy(view, view, in_sem.at[i % 2, n]).wait()
        pl.when(i >= 2)(lambda: store_copy(i - 2).wait())
        gbuf[low, :] = gbuf[high, :]
        pbuf[low, :] = pbuf[high, :]
        place(gbuf, ROWS, ROWS, lambda: gin[i % 2])
        scale, inv1, inv2 = [cbuf[n, :1] for n in STATE]
        for j in range(ROWS // size):
            first, count = size * 128 * j, size * 128
            h = window(gbuf, rho, j) * scale
            m, v, p = [sin[flat(i, n, first, count)].reshape(size, 128) for n in STATE]
            m1 = b1 * m + (1.0 - b1) * h
            v1 = b2 * v + (1.0 - b2) * (h * h)
            pos = me * SHARE + i * BLK + first + sub * 128 + lane
            decay = jnp.where(pos < DECAY_LEN, wd * p, 0.0)
            u = (m1 * inv1) / (jnp.sqrt(v1 * inv2) + ADAM_EPS) + decay
            p1 = p - lr * u
            place(pbuf, ROWS + size * j, size, lambda: p1)
            sout[pl.ds(pl.multiple_of(i % 2 * BLK + first, 1024), count)] = p1.reshape(count)

            @pl.when(i < OWN)
            def _():
                for n, value in enumerate((m1, v1)):
                    outs[n][pl.ds(pl.multiple_of(i * BLK + first, 1024), count)] = value.reshape(count)

        pl.when(i < OWN)(lambda: store_copy(i).start())

    def finish(i):
        j = i - 1
        for k in range(ROWS // size):
            fbuf[pl.ds(size * k, size), :] = window(pbuf, sigma, k)
        b = own_start(me) + j

        def emit(t, value):
            obuf[j % SLOTS, t] = value.astype(jnp.bfloat16)
        is_row, is_gate, is_q, is_kv = kind_of(b)
        pl.when(is_row)(functools.partial(joined_to_rows, fbuf, emit))
        pl.when(is_gate)(functools.partial(joined_to_transposed, "gate", fbuf, tbuf, emit))
        pl.when(is_q)(functools.partial(joined_to_transposed, "q", fbuf, tbuf, emit))
        pl.when(is_kv)(functools.partial(joined_to_transposed, "kv", fbuf, tbuf, emit))
        block_start(j)

    def view(h, share, q, count):
        return o.at[pl.ds(share * GATHERED + q * PART, count), h]

    def copy(h, share, q, count, send, recv, device):
        span_ = view(h, share, q, count)
        pltpu.make_async_remote_copy(
            src_ref=span_, dst_ref=span_, send_sem=send, recv_sem=recv,
            device_id=(device,), device_id_type=MESH).start()

    def to_partner(h, which, q, count):
        share = (me, near[h], near[1 - h], far)[which]
        copy(h, share, q, count, p_send.at[h, which], p_recv.at[h, which, q], partner)

    def second_hop(h, which, q, count):
        share = (me, near[h])[which]
        copy(h, share, q, count, s_send.at[h, which], s_recv.at[h, which, q], near[1 - h])

    def arrived(h, count, sem):
        span_ = view(h, 0, 0, count)
        pltpu.make_async_copy(span_, span_, sem).wait()

    def stored(q, count):
        for n in range(2 * count):
            block_wait(2 * PART * q + n)

    def send_own(q, count):
        for h in HALVES:
            copy(h, me, q, count, f_send.at[h], f_recv.at[h, q], near[h])
            second_hop(h, 0, q, count)
        for h in HALVES:
            to_partner(h, 0, q, count)

    def forward_near(q, count):
        for h in HALVES:
            arrived(h, count, f_recv.at[h, q])
            second_hop(h, 1, q, count)
            to_partner(h, 1, q, count)
        for h in HALVES:
            arrived(h, count, s_recv.at[h, 0, q])
            to_partner(h, 2, q, count)

    def forward_far(q, count):
        for h in HALVES:
            arrived(h, count, s_recv.at[h, 1, q])
            to_partner(h, 3, q, count)

    one = jnp.ones((8, 128), jnp.float32)

    def power(b):
        square = b * b
        cube = b * square
        return cube * (square * square)

    start_loads(jnp.int32(0))
    norm = jnp.sqrt(jnp.sum(nrm_ref[...], keepdims=True) * (1.0 / 64.0))
    clip = jnp.minimum(1.0, (one * max_norm) / (norm + CLIP_EPS))
    cbuf[0] = clip * 0.125
    cbuf[1] = one / (one * (1.0 - power(b1)))
    cbuf[2] = one / (one * (1.0 - power(b2)))
    g_copy(0, 2).start()
    g_copy(0, 2).wait()
    place(gbuf, ROWS, ROWS, lambda: gin[2])

    whole = (OWN_HALF - 1) // PART
    handed = GATHERED // PART
    step(jnp.int32(0))

    def inner(n, q):
        i = 2 * PART * q + n + 1
        step(i)
        finish(i)

        @pl.when((n == 0) & (q >= 1))
        def _():
            stored(q - 1, PART)
            pl.when(q <= handed)(lambda: send_own(q - 1, PART))
        return q

    def outer(q, carry):
        lax.fori_loop(0, 2 * PART, inner, q)
        pl.when((q >= NEAR_LAG) & (q - NEAR_LAG < handed))(lambda: forward_near(q - NEAR_LAG, PART))
        pl.when((q >= FAR_LAG) & (q - FAR_LAG < handed))(lambda: forward_far(q - FAR_LAG, PART))
        return carry

    lax.fori_loop(0, whole, outer, 0)
    stored(whole - 1, PART)

    def last(i, carry):
        step(i)
        finish(i)
        return carry

    lax.fori_loop(OWN - 1, OWN + 1, last, 0)
    stored(whole, 1)

    def rest(fn, first):
        def body(q, carry):
            fn(q, PART)
            return carry
        lax.fori_loop(min(first, handed), handed, body, 0)
    rest(forward_near, whole - NEAR_LAG)
    rest(forward_far, whole - FAR_LAG)

    store_copy(OWN - 1).wait()

    def from_partner(q, count):
        for h in HALVES:
            for which in ALL:
                arrived(h, count, p_recv.at[h, which, q])
    rest(from_partner, 0)
    for h in HALVES:
        arrived(h, GATHERED, f_send.at[h])
        for which in HALVES:
            arrived(h, GATHERED, s_send.at[h, which])
        for which in ALL:
            arrived(h, GATHERED, p_send.at[h, which])


def run_update(hyper, nrm, g, state, tails):
    f32, bf16, dma = jnp.float32, jnp.bfloat16, pltpu.SemaphoreType.DMA
    any_spec = pl.BlockSpec(memory_space=pl.ANY)
    chunks = GATHERED // PART
    rows = pltpu.VMEM((2 * ROWS + 8, 128), f32)
    flat = pltpu.VMEM((6 * BLK,), f32)
    return pl.pallas_call(
        update_kernel,
        in_specs=[pl.BlockSpec(memory_space=pltpu.SMEM), pl.BlockSpec(memory_space=pltpu.VMEM)] + [any_spec] * 7,
        out_specs=[pl.BlockSpec(memory_space=pltpu.VMEM)] * PAIR + [any_spec] * STATE[-1] + [any_spec],
        out_shape=[pltpu.VMEM((OWN * BLK,), f32)] * PAIR + [jax.ShapeDtypeStruct((OWN * BLK,), f32)]
        + [jax.ShapeDtypeStruct(n + TILE, bf16) for n in ((GROUP * GATHERED, 2), (LATE,))],
        scratch_shapes=[
            rows, rows, pltpu.VMEM((ROWS, 128), f32), pltpu.VMEM((3, 128, 128), f32),
            pltpu.VMEM((3, 8, 128), f32), pltpu.VMEM((3, ROWS, 128), f32), flat, pltpu.VMEM((PAIR * BLK,), f32),
            pltpu.VMEM((SLOTS,) + TILE, bf16),
            dma((3, 4)), dma((PAIR,)), dma((SLOTS,)), dma((PAIR,)), dma((PAIR, chunks)), dma((PAIR, 2)),
            dma((PAIR, 2, chunks)), dma((PAIR, 4)), dma((PAIR, 4, chunks))],
        compiler_params=pltpu.CompilerParams(collective_id=1, has_side_effects=True, vmem_limit_bytes=6 * 2**20),
        name="update_gather",
    )(hyper, nrm, g, *state, *tails)


def pack(grads):
    embed, q, k, v, out, gate, up, down, norms, qk = [g[0] for g in grads]

    def rows(a):
        return a.reshape(-1, 8, COLS, 128).transpose(0, 2, 1, 3)

    def grid(a):
        layers, wide, high = a.shape
        return a.transpose(0, 2, 1).reshape(layers, high // 8, 8, COLS, 128).transpose(0, 1, 3, 2, 4)

    tail = jnp.concatenate([norms.reshape(-1), qk.reshape(-1)])
    tail = jnp.pad(tail, (0, TAIL_BLOCKS * BLK - tail.shape[0]))
    return rows(embed), grid(q), grid(k), grid(v), rows(out), grid(gate), grid(up), rows(down), rows(tail.reshape(-1, 4608))


def block_runs(b0, b1):
    out = []
    for r in range(GROUP):
        start = own_start(r)
        lo, hi = max(b0, start), min(b1, own_start(r + 1), start + 2 * GATHERED)
        if lo < hi:
            out.append((r * 2 * GATHERED + lo - start, lo - b0, hi - lo))
    return out


def is_rows(kind):
    return kind in (0, 4, 7, 8)


def unpack_kernel(kinds, o, *refs):
    outs, (buf, in_sem, out_sem) = refs[:len(kinds)], refs[len(kinds):]

    def rows_out(ref, first):
        def store(slot, count):
            pltpu.make_async_copy(
                buf.at[slot, pl.ds(0, count)], ref.at[pl.ds(first, count)], out_sem.at[slot]).start()
        return store

    def grid_out(ref, layer):
        def store(slot, count):
            def one(rt, z):
                pltpu.make_async_copy(buf.at[slot, :, rt], ref.at[layer, rt], out_sem.at[slot]).start()
                return z
            lax.fori_loop(0, COLS, one, 0)
        return store

    def cols_out(ref):
        high = ref.shape[1]
        wide = COLS // high

        def store(slot, count):
            def one(n, z):
                for rt in range(high):
                    pltpu.make_async_copy(
                        buf.at[slot, n, pl.ds(wide * rt, wide)],
                        ref.at[n // high, rt, pl.ds((n % high) * wide, wide)], out_sem.at[slot]).start()
                return z
            lax.fori_loop(0, count, one, 0)
        return store

    jobs = []
    for kind, ref in zip(kinds, outs):
        first = EDGES[kind]
        if is_rows(kind):
            count = ref.shape[0]
            for lo in range(0, count, COLS):
                jobs.append((first + lo, min(COLS, count - lo), rows_out(ref, lo)))
        elif ref.shape[1] == COLS:
            for layer in range(ref.shape[0]):
                jobs.append((first + COLS * layer, COLS, grid_out(ref, layer)))
        else:
            jobs.append((first, EDGES[kind + 1] - first, cols_out(ref)))
    depth = buf.shape[0]

    def load(n):
        b0, count, _ = jobs[n]
        for first, at, size in block_runs(b0, b0 + count):
            pltpu.make_async_copy(
                o.at[pl.ds(first, size)], buf.at[n % depth, pl.ds(at, size)], in_sem.at[n % depth]).start()

    def wait(n, count, sem):
        if count:
            view = buf.at[n % depth, pl.ds(0, count)]
            pltpu.make_async_copy(view, view, sem.at[n % depth]).wait()

    def loaded(n):
        b0, count, _ = jobs[n]
        return sum(size for _, _, size in block_runs(b0, b0 + count))

    lead = depth // 2
    for n in range(len(jobs) + lead):
        if n < len(jobs):
            if n >= depth:
                wait(n - depth, jobs[n - depth][1], out_sem)
            load(n)
        if n >= lead:
            wait(n - lead, loaded(n - lead), in_sem)
            jobs[n - lead][2]((n - lead) % depth, jobs[n - lead][1])
    for n in range(len(jobs) - depth, len(jobs)):
        wait(n, jobs[n][1], out_sem)


def late_kernel(*refs):
    count = len(EDGES) - 1
    late, outs = refs[:GROUP], refs[GROUP + count:GROUP + 2 * count]
    buf, in_sem, out_sem = refs[GROUP + 2 * count:]
    me = lax.axis_index("dp")
    y, x, c, _, _ = positions(me)
    for k in range(GROUP):
        pltpu.make_async_copy(late[k], buf.at[k], in_sem).start()
    pltpu.make_async_copy(buf, buf, in_sem).wait()

    def differs(bit, mine):
        return 1 - mine if bit else mine

    for r in range(GROUP):
        ry, rx, rc, _, _ = positions(r)
        k = dev(differs(ry, y), differs(rx, x), differs(rc, c))
        start, end = own_start(r) + 2 * GATHERED, own_start(r + 1)
        for kind, ref in enumerate(outs):
            lo, hi = max(start, EDGES[kind]), min(end, EDGES[kind + 1])
            if lo >= hi:
                continue
            if is_rows(kind):
                pltpu.make_async_copy(
                    buf.at[k, pl.ds(lo - start, hi - lo)], ref.at[pl.ds(lo - EDGES[kind], hi - lo)],
                    out_sem).start()
                continue
            assert ref.shape[1] == COLS
            for layer in range(ref.shape[0]):
                base = EDGES[kind] + COLS * layer
                at, to = max(lo, base), min(hi, base + COLS)
                if at < to:
                    def one(rt, z, ref=ref, layer=layer, k=k, n=at - start, col=at - base, tiles=to - at):
                        pltpu.make_async_copy(
                            buf.at[k, pl.ds(n, tiles), rt], ref.at[layer, rt, pl.ds(col, tiles)],
                            out_sem).start()
                        return z
                    lax.fori_loop(0, COLS, one, 0)
    for r in range(GROUP):
        view = buf.at[r, pl.ds(0, own_start(r + 1) - own_start(r) - 2 * GATHERED)]
        pltpu.make_async_copy(view, view, out_sem).wait()


def out_views(shapes):
    views = []
    for kind in range(len(EDGES) - 1):
        if is_rows(kind):
            views.append((EDGES[kind + 1] - EDGES[kind],) + TILE)
        else:
            views.append((shapes[kind][0], shapes[kind][2] // 8) + TILE)
    return views


def run_unpack(o, kinds, views):
    bf16, dma, depth = jnp.bfloat16, pltpu.SemaphoreType.DMA, 4
    any_spec = pl.BlockSpec(memory_space=pl.ANY)
    size = sum(math.prod(views[kind]) for kind in kinds)
    return pl.pallas_call(
        functools.partial(unpack_kernel, kinds),
        out_shape=[jax.ShapeDtypeStruct(views[kind], bf16) for kind in kinds],
        in_specs=[any_spec], out_specs=[any_spec] * len(kinds),
        scratch_shapes=[pltpu.VMEM((depth, COLS) + TILE, bf16), dma((depth,)), dma((depth,))],
        cost_estimate=pl.CostEstimate(flops=size * 1000, bytes_accessed=size * 4, transcendentals=0),
        compiler_params=pltpu.CompilerParams(vmem_limit_bytes=12 * 2**20),
        name="unpack",
    )(o)


def run_late(late, params):
    bf16, dma, count = jnp.bfloat16, pltpu.SemaphoreType.DMA, len(params)
    any_spec = pl.BlockSpec(memory_space=pl.ANY)
    return pl.pallas_call(
        late_kernel, out_shape=[jax.ShapeDtypeStruct(a.shape, bf16) for a in params],
        in_specs=[any_spec] * (GROUP + count), out_specs=[any_spec] * count,
        input_output_aliases={GROUP + n: n for n in range(count)},
        scratch_shapes=[pltpu.VMEM((GROUP, LATE) + TILE, bf16), dma, dma],
        compiler_params=pltpu.CompilerParams(vmem_limit_bytes=12 * 2**20),
        name="unpack_late",
    )(*late, *params)


def to_shapes(outs, shapes):
    def from_rows(a, shape):
        return a.swapaxes(1, 2).reshape(shape)

    def from_grid(a, shape):
        layers, wide, high = shape
        return a.swapaxes(2, 3).reshape(layers, high, wide).swapaxes(1, 2)
    params = [(from_grid if len(a.shape) > 4 else from_rows)(a, s) for a, s in zip(outs[:8], shapes)]
    tail = from_rows(outs[8], (-1,))
    size = math.prod(shapes[8])
    params.append(tail[:size].reshape(shapes[8]))
    params.append(tail[size:size + math.prod(shapes[9])].reshape(shapes[9]))
    return tuple(params)


def swap(a, bit):
    return lax.ppermute(a, "dp", [(r, r ^ bit) for r in range(GROUP)])


def solution(mesh):
    group_size = mesh.shape["dp"]
    assert group_size == GROUP

    def local_update(*arrays):
        grads = arrays[:GRAD_COUNT]
        first_part, second_part, master_part, hyper_params = arrays[GRAD_COUNT:]
        state = (first_part, second_part, master_part)
        shapes = [grad_arr.shape[1:] for grad_arr in grads]

        heads = jnp.concatenate([s[:BLK] for s in state])
        heads = lax.ppermute(heads, "dp", [(r + 1, r) for r in range(GROUP - 1)])
        rest = 2 * BLK - (SHARE - 121 * BLK) - BLK
        tails = [jnp.concatenate([s[121 * BLK:], heads[n * BLK:(n + 1) * BLK], jnp.zeros((rest,), s.dtype)])
                 for n, s in enumerate(state)]

        g, nrm = run_reduce(pack(grads))
        *moved, o, own = run_update(hyper_params, nrm, g, state, tails)
        own, moved[0] = lax.optimization_barrier((own, moved[0][:SHARE]))
        near = [swap(own, bit) for bit in (2, 4, 6)]
        first = swap(own, 1)
        o, *moved = lax.optimization_barrier([o, moved[0]] + [a[:SHARE] for a in moved[1:]])
        o = o.reshape((-1,) + TILE)
        views = out_views(shapes)
        early_kinds, other_kinds = (0, 4, 7, 5), (1, 2, 3, 6, 8)
        early = run_unpack(o, early_kinds, views)
        o, near, early = lax.optimization_barrier((o, near, early))
        cross = [swap(a, 1) for a in near]
        other = run_unpack(o, other_kinds, views)
        cross, other = lax.optimization_barrier((cross, other))
        found = dict(zip(early_kinds + other_kinds, list(early) + list(other)))
        late = [own, first]
        for a, b in zip(near, cross):
            late += [a, b]
        outs = run_late(late, [found[kind] for kind in range(len(views))])
        return to_shapes(outs, shapes) + tuple(moved)

    in_specs = tuple([P("dp")] * GRAD_COUNT + [P("dp"), P("dp"), P("dp"), P()])
    out_specs = tuple([P()] * GRAD_COUNT + [P("dp"), P("dp"), P("dp")])
    return jax.shard_map(local_update, mesh=mesh, in_specs=in_specs, out_specs=out_specs, check_vma=False)
```
